32 devices in a mesh: gx: 8 (over z, x), gy: 4 (over y, core).
Axes of the slice: x: 2, y: 2, z: 4, core: 2. Of those that a mesh axis runs over, the one named last changes fastest.
Arguments:
- pressure: float32 [256, 128, 128], P('gx', 'gy'), may hold values from -6 to 6
- depth: float32 [256, 128, 128], P('gx', 'gy'), may hold values from -6 to 6
- saturation: float32 [2, 256, 128, 128], P(None, 'gx', 'gy'), may hold values from 0.05 to 0.45
- permeability: float32 [3, 256, 128, 128], P(None, 'gx', 'gy'), may hold values from 0.1 to 10
- pore_volume: float32 [256, 128, 128], P('gx', 'gy'), may hold values from 0.5 to 2
- fault_pairs: int32 [1024, 3], P(('gx', 'gy')), may hold values from 0 to 1023, as said below
- fault_kind: int32 [1024], P(('gx', 'gy')), may hold values from 0 to 15
- fault_count: int32 [32], P(('gx', 'gy')), may hold values from 8 to 32, as said below
- fault_table: float32 [16, 128], replicated, may hold values from 0.2 to 2
Outputs:
- saturation_next: float32 [3, 256, 128, 128], P(None, 'gx', 'gy')
The draws below stay inside these ranges and needn't reach their ends.
Inputs may be any that keep to these rules, and one draw needn't show every extreme that they name: `fault_pairs`: each device holds 32 rows. Column 0 and column 2 are areal column numbers a * 32 + b of the source and target device. Column 1 is the target device i2 * 4 + j2, which lies within one index of the source device along gx and along gy, counted cyclically. Among one device's 32 rows at most 4 name the same target device, and on every device some target device is named by exactly 4 rows. Rows 0 to fault_count - 1 of a device are live; some device has 32 live rows.
All inputs are finite; a program needn't handle non-finite values.
Results may differ from the reference program's by a relative error of at most 0.0003.
Values sent between devices are 32-bit elements; how exact they have to be, the bound alone decides.
No kernel may reach another device: no remote copies, remote signals or barrier semaphores. Data moves between devices by JAX's collectives and lax.ppermute only.
A program may use at most 64 MiB of HBM per device.

```python
import math
import jax
import jax.numpy as jnp
from jax import lax

CX = 32
CY = 32
NZ = 128
FB = 32
CAP = 4
NTAB = 16
NX = 256
NY = 128
N_GX = 8
N_GY = 4


def draw_fault_pairs(key, part):
    devices = N_GX * N_GY

    def one_device(device_key, device):
        order = jax.random.permutation(jax.random.fold_in(device_key, 1), 9 * CAP)[:FB].astype(jnp.int32)
        near = order // CAP
        step_x = near // 3 - 1
        step_y = near % 3 - 1
        home_x = device // N_GY
        home_y = device % N_GY
        target = (home_x + step_x) % N_GX * N_GY + (home_y + step_y) % N_GY
        source = jax.random.randint(jax.random.fold_in(device_key, 2), (FB,), 0, CX * CY, dtype=jnp.int32)
        landing = jax.random.randint(jax.random.fold_in(device_key, 3), (FB,), 0, CX * CY, dtype=jnp.int32)
        return jnp.stack([source, target.astype(jnp.int32), landing], axis=1)
    keys = jax.random.split(jax.random.fold_in(key, 11), devices)
    device_ids = jnp.arange(devices, dtype=jnp.int32)
    return jax.vmap(one_device)(keys, device_ids).reshape(devices * FB, 3)


def draw_fault_count(key, part):
    devices = N_GX * N_GY
    levels = jax.random.randint(jax.random.fold_in(key, 21), (devices,), 0, 3, dtype=jnp.int32)
    counts = jnp.where(levels == 0, FB, jnp.where(levels == 1, FB // 2, FB // 4)).astype(jnp.int32)
    busiest = jax.random.randint(jax.random.fold_in(key, 22), (), 0, devices, dtype=jnp.int32)
    return jnp.where(jnp.arange(devices, dtype=jnp.int32) == busiest, FB, counts).astype(jnp.int32)


def set_ends(entries, own_key, low, largest):
    index_at = [jax.random.randint(jax.random.fold_in(own_key, axis), (), 0, length) for axis, length in enumerate(entries.shape)]
    widest = entries.shape.index(max(entries.shape))
    beside = index_at[:widest] + [(index_at[widest] + 1) % entries.shape[widest]] + index_at[widest + 1:]
    return entries.at[tuple(index_at)].set(low).at[tuple(beside)].set(largest)


def shard_levels(key, dims, cuts, smallest, top_value):
    loudness, own = 1.0, jax.random.fold_in(key, 6)
    for dim, parts in cuts:
        draws = jnp.exp(jax.random.uniform(jax.random.fold_in(own, dim), (parts,), jnp.float32, smallest / len(cuts), top_value / len(cuts)))
        loudness = loudness * jnp.repeat(draws, dims[dim] // parts).reshape([-1 if axis == dim else 1 for axis in range(len(dims))])
    return loudness


def normal_values(own_key, dims, spread, reach, cuts=(), held_as=jnp.bfloat16):
    factor_of = shard_levels(own_key, dims, cuts, -0.22, 0.18) if cuts else 1.0
    values = jax.random.normal(own_key, dims, jnp.float32) * spread * factor_of
    return jnp.minimum(jnp.maximum(values, -reach), reach).astype(held_as)


def setup_inputs(seed: int = 0) -> dict:
    streams_of = jax.random.split(jax.random.key(seed), 10)
    pressure = normal_values(streams_of[0], (NX, NY, NZ), 1.0, 6.0, ((0, 8), (1, 4)), jnp.float32)
    depth = normal_values(streams_of[1], (NX, NY, NZ), 1.0, 6.0, ((0, 8), (1, 4)), jnp.float32)
    saturation = jnp.clip(0.05 + 0.39999999 * jax.random.uniform(streams_of[2], (2, NX, NY, NZ), jnp.float32) ** shard_levels(streams_of[2], (2, NX, NY, NZ), ((1, 8), (2, 4)), -0.2, 0.2), 0.05, 0.45)
    permeability = jnp.clip(jnp.exp(math.log(10.0) - 4.6051702 * jax.random.uniform(streams_of[3], (3, NX, NY, NZ), jnp.float32) ** shard_levels(streams_of[3], (3, NX, NY, NZ), ((1, 8), (2, 4)), -0.2, 0.2)), 0.1, 10.0)
    pore_volume = jnp.clip(jnp.exp(math.log(2.0) - 1.3862944 * jax.random.uniform(streams_of[4], (NX, NY, NZ), jnp.float32) ** shard_levels(streams_of[4], (NX, NY, NZ), ((0, 8), (1, 4)), -0.2, 0.2)), 0.5, 2.0)
    fault_pairs = draw_fault_pairs(jax.random.fold_in(streams_of[9], 71), 0)
    fault_kind = set_ends(jax.random.randint(streams_of[6], (N_GX * N_GY * FB,), 0, NTAB), jax.random.fold_in(streams_of[6], 1), 0, NTAB - 1).astype(jnp.int32)
    fault_count = draw_fault_count(jax.random.fold_in(streams_of[9], 71), 0)
    fault_table = jnp.clip(jnp.exp(jax.random.uniform(streams_of[8], (NTAB, NZ), jnp.float32, math.log(0.2), math.log(2.0))), 0.2, 2.0)
    return dict(pressure=pressure, depth=depth, saturation=saturation, permeability=permeability, pore_volume=pore_volume, fault_pairs=fault_pairs, fault_kind=fault_kind, fault_count=fault_count, fault_table=fault_table)


VISCOSITY = (0.5, 1.0, 0.25)
DENSITY = (1.0, 0.8, 0.25)
step_length = 0.2


def mobility(sat_water, sat_oil):
    sat_gas = 1.0 - sat_water - sat_oil
    return (sat_water * sat_water / VISCOSITY[0], sat_oil * sat_oil / VISCOSITY[1], sat_gas * sat_gas / VISCOSITY[2])


def harmonic(first, second):
    return 2.0 * first * second / (first + second)


def phase_flux(press_low, depth_low, mobile_low, press_high, depth_high, mobile_high, trans):
    flows = []
    for phase in range(3):
        drive = (press_low - press_high) - DENSITY[phase] * (depth_low - depth_high)
        upwind = jnp.where(drive > 0.0, mobile_low[phase], mobile_high[phase])
        flows.append(trans * upwind * drive)
    return jnp.stack(flows, axis=-2)


def consecutive(array, axis, start):
    return lax.slice_in_dim(array, start, array.shape[axis] - 1 + start, axis=axis)


def face_flows(press, height, mobile, perm, axis):
    def lower(array):
        return consecutive(array, axis, 0)

    def upper(array):
        return consecutive(array, axis, 1)

    return phase_flux(lower(press), lower(height), tuple(lower(m) for m in mobile),
                      upper(press), upper(height), tuple(upper(m) for m in mobile),
                      harmonic(lower(perm), upper(perm)))


def reference(pressure, depth, saturation, permeability, pore_volume, fault_pairs, fault_kind, fault_count, fault_table):
    sat_water = saturation[0]
    sat_oil = saturation[1]
    mobile = mobility(sat_water, sat_oil)
    flow_x = jnp.pad(face_flows(pressure, depth, mobile, permeability[0], 0), ((1, 1), (0, 0), (0, 0), (0, 0)))
    flow_y = jnp.pad(face_flows(pressure, depth, mobile, permeability[1], 1), ((0, 0), (1, 1), (0, 0), (0, 0)))
    flow_z = jnp.pad(face_flows(pressure, depth, mobile, permeability[2], 2), ((0, 0), (0, 0), (0, 0), (1, 1)))
    net = (flow_x[1:] - flow_x[:-1]) + (flow_y[:, 1:] - flow_y[:, :-1]) + (flow_z[..., 1:] - flow_z[..., :-1])
    devices = N_GX * N_GY
    pairs = fault_pairs.reshape(devices, FB, 3)
    device = jnp.arange(devices, dtype=jnp.int32)[:, None]
    home_x = device // N_GY
    home_y = device % N_GY
    source = ((home_x * CX + pairs[..., 0] // CY) * NY + home_y * CY + pairs[..., 0] % CY).reshape(-1)
    target = pairs[..., 1]
    dest = (((target // N_GY) * CX + pairs[..., 2] // CY) * NY + (target % N_GY) * CY + pairs[..., 2] % CY).reshape(-1)
    live = (jnp.arange(FB, dtype=jnp.int32)[None, :] < fault_count[:, None]).reshape(-1)
    trans = fault_table[fault_kind] * live[:, None].astype(jnp.float32)
    press_flat = pressure.reshape(NX * NY, NZ)
    depth_flat = depth.reshape(NX * NY, NZ)
    mobile_flat = tuple(m.reshape(NX * NY, NZ) for m in mobile)
    fault_flow = phase_flux(press_flat[source], depth_flat[source], tuple(m[source] for m in mobile_flat),
                            press_flat[dest], depth_flat[dest], tuple(m[dest] for m in mobile_flat), trans)
    net_flat = net.reshape(NX * NY, 3, NZ).at[source].add(fault_flow).at[dest].add(-fault_flow)
    net = net_flat.reshape(NX, NY, 3, NZ)
    sat_gas = 1.0 - sat_water - sat_oil
    return jnp.stack([current - step_length * net[:, :, phase, :] / pore_volume
                      for phase, current in enumerate((sat_water, sat_oil, sat_gas))], axis=0)
```

```python
import functools

import jax
import jax.numpy as jnp
from jax import lax
from jax.experimental import pallas as pl
from jax.experimental.pallas import tpu as pltpu
from jax.sharding import PartitionSpec as P

CAP = 4
FIELDS = 5
BLOCK = CAP * FIELDS
META = 3 * BLOCK
ROWS = 64
FLOW = 3 * CAP
BACK = 40

VISCOSITY = (0.5, 1.0, 0.25)
DENSITY = (1.0, 0.8, 0.25)
STEP = 0.2


VMEM = pltpu.VMEM
HBM = pltpu.HBM
SMEM = pltpu.SMEM


def spec(space):
    return pl.BlockSpec(memory_space=space)


def params(limit=6):
    return pltpu.CompilerParams(vmem_limit_bytes=limit * 2**20)


def cost(flops):
    return pl.CostEstimate(flops=flops, bytes_accessed=flops // 64, transcendentals=0)


def mobility(water, oil):
    gas = 1.0 - water - oil
    return (
        water * water * (1.0 / VISCOSITY[0]),
        oil * oil * (1.0 / VISCOSITY[1]),
        gas * gas * (1.0 / VISCOSITY[2]),
    )


def harmonic(first, second):
    return (first * second + first * second) / (first + second)


def flux(low, high, trans):
    dp = low[0] - high[0]
    dd = low[1] - high[1]
    flows = []
    for phase in range(3):
        drive = dp - DENSITY[phase] * dd if DENSITY[phase] != 1.0 else dp - dd
        up = jnp.where(drive > 0.0, low[2 + phase], high[2 + phase])
        flows.append(trans * drive * up)
    return flows


def pack_kernel(
    nx, ny, cx, cy,
    pairs_ref, kind_ref, count_ref, table_ref, press_h, depth_h, sat_h, perm_h,
    press_f, depth_f, sat_f,
    own, msg_a, msg_b, hxa, hxb, hya, hyb, press, depth, sat,
    pairs_s, kind_s, count_s, slot_s, seen_s, src_s, knd_s, liv_s, lnd_s, table,
    sem_i, sem_s, sem_h,
):
    ints = [
        pltpu.make_async_copy(pairs_ref, pairs_s, sem_i.at[0]),
        pltpu.make_async_copy(kind_ref, kind_s, sem_i.at[1]),
        pltpu.make_async_copy(count_ref, count_s, sem_i.at[2]),
        pltpu.make_async_copy(table_ref, table, sem_i.at[3]),
    ]
    for copy in ints:
        copy.start()
    bulk = [
        pltpu.make_async_copy(press_f, press, sem_s.at[0]),
        pltpu.make_async_copy(depth_f, depth, sem_s.at[1]),
        pltpu.make_async_copy(sat_f, sat, sem_s.at[2]),
    ]
    for copy in bulk:
        copy.start()
    home_x = lax.axis_index("gx")
    home_y = lax.axis_index("gy")
    even_x = lax.rem(home_x, 2) == 0
    even_y = lax.rem(home_y, 2) == 0
    row_up = jnp.where(even_x, cx - 1, 0)
    row_dn = jnp.where(even_x, 0, cx - 1)
    col_up = jnp.where(even_y, cy - 1, 0)
    col_dn = jnp.where(even_y, 0, cy - 1)
    halos = []
    sources = (press_h, depth_h, sat_h.at[0], sat_h.at[1])
    for field in range(5):
        src = sources[field] if field < 4 else perm_h.at[0]
        halos.append((src.at[row_up], hxa.at[field]))
        halos.append((src.at[row_dn], hxb.at[field]))
        src = sources[field] if field < 4 else perm_h.at[1]
        halos.append((src.at[:, col_up, :], hya.at[field]))
        halos.append((src.at[:, col_dn, :], hyb.at[field]))
    halos = [
        pltpu.make_async_copy(src, dst, sem_h.at[k]) for k, (src, dst) in enumerate(halos)
    ]
    for copy in halos:
        copy.start()
    for step_x in (0, 1, -1):
        to_x = lax.rem(home_x + step_x + nx, nx)
        tx = step_x % 3
        for step_y in (0, 1, -1):
            to_y = lax.rem(home_y + step_y + ny, ny)
            if step_y == 0:
                ty = 0
            else:
                ty = jnp.where(even_y == (step_y == 1), 1, 2)
            slot_s[to_x * ny + to_y] = (ty * 3 + tx) * CAP
    for k in range(9 * CAP):
        seen_s[k] = 0
        src_s[k] = 0
        knd_s[k] = 0
        liv_s[k] = 0
        lnd_s[k] = 0
    for copy in ints:
        copy.wait()
    count = count_s[0, 0]
    for r in range(pairs_s.shape[1]):
        base = slot_s[pairs_s[1, r]]
        rank = seen_s[base]
        seen_s[base] = rank + 1
        position = base + rank
        src_s[position] = pairs_s[0, r]
        lnd_s[position] = pairs_s[2, r]
        knd_s[position] = kind_s[r]
        liv_s[position] = jnp.where(r < count, 1, 0)
    lane = lax.broadcasted_iota(jnp.int32, (1, own.shape[1]), 1)
    messages = (own, msg_a, msg_b)
    origin = jnp.zeros(lane.shape, jnp.int32)
    for ty in range(3):
        out = messages[ty]
        for tx in range(3):
            meta = jnp.zeros(lane.shape, jnp.int32)
            for rank in range(CAP):
                k = (ty * 3 + tx) * CAP + rank
                meta = jnp.where(lane == rank, lnd_s[k], meta)
                origin = jnp.where(lane == k, src_s[k], origin)
                trans = table[pl.ds(knd_s[k], 1), :]
                alive = liv_s[k].astype(jnp.float32)
                out[tx * BLOCK + 4 * CAP + rank : tx * BLOCK + 4 * CAP + rank + 1, :] = trans * alive
            out[META + tx : META + tx + 1, :] = meta.astype(jnp.float32)
        out[META + 3 : META + 4, :] = jnp.zeros(lane.shape, jnp.float32)
    own[META + 3 : META + 4, :] = origin.astype(jnp.float32)
    for copy in bulk:
        copy.wait()
    for ty in range(3):
        out = messages[ty]
        for tx in range(3):
            for rank in range(CAP):
                k = (ty * 3 + tx) * CAP + rank
                col = src_s[k]
                at = tx * BLOCK + rank
                out[at : at + 1, :] = press[pl.ds(col, 1), :]
                out[at + CAP : at + CAP + 1, :] = depth[pl.ds(col, 1), :]
                out[at + 2 * CAP : at + 2 * CAP + 1, :] = sat[0, pl.ds(col, 1), :]
                out[at + 3 * CAP : at + 3 * CAP + 1, :] = sat[1, pl.ds(col, 1), :]
    for copy in halos:
        copy.wait()


def load_state(press, depth, sat, rows):
    water, oil = sat[0, rows, :], sat[1, rows, :]
    return (press[rows, :], depth[rows, :]) + mobility(water, oil), water, oil


def stencil_kernel(cx, cy, first, last, *refs):
    if first == 0:
        press, depth, sat, perm, pore, out = refs
    else:
        press, depth, sat, perm, pore, _, out = refs
    lanes = press.shape[1]
    lane = lax.broadcasted_iota(jnp.int32, (8, lanes), 1)
    sub = lax.broadcasted_iota(jnp.int32, (8, lanes), 0)
    chunks = cy // 8

    def at(a, c, shift=0):
        return pl.ds(pl.multiple_of(a * cy, 8) + (c * 8 + shift), 8)

    def flow_x(a, c, low, scale):
        rows = at(a + 1, c)
        high, _, _ = load_state(press, depth, sat, rows)
        trans = harmonic(perm[0, at(a, c), :], perm[0, rows, :])
        return flux(low, high, trans)

    def one_row(a, carry, top):
        out_carry = []
        below = None
        for c in range(chunks):
            rows = at(a, c)
            mine, water, oil = load_state(press, depth, sat, rows)
            if top:
                net = [-carry[3 * c + f] for f in range(3)]
            else:
                up = flow_x(a, c, mine, None)
                out_carry += up
                net = [up[f] - carry[3 * c + f] for f in range(3)]
            ky = perm[1, rows, :]
            if c < chunks - 1:
                rows_up = at(a, c, 1)
                high, _, _ = load_state(press, depth, sat, rows_up)
                trans = harmonic(ky, perm[1, rows_up, :])
            else:
                high = tuple(pltpu.roll(v, 7, 0) for v in mine)
                trans = jnp.where(sub < 7, harmonic(ky, pltpu.roll(ky, 7, 0)), 0.0)
            flow = flux(mine, high, trans)
            for f in range(3):
                back = pltpu.roll(flow[f], 1, 0)
                first_row = jnp.zeros_like(back) if c == 0 else below[f]
                net[f] = net[f] + (flow[f] - jnp.where(sub == 0, first_row, back))
            below = [pltpu.roll(flow[f], 1, 0) for f in range(3)]
            kz = perm[2, rows, :]
            high = tuple(pltpu.roll(v, lanes - 1, 1) for v in mine)
            trans = jnp.where(lane < lanes - 1, harmonic(kz, pltpu.roll(kz, lanes - 1, 1)), 0.0)
            flow = flux(mine, high, trans)
            for f in range(3):
                net[f] = net[f] + (flow[f] - pltpu.roll(flow[f], 1, 1))
            scale = STEP / pore[rows, :]
            gas = 1.0 - water - oil
            for f, now in enumerate((water, oil, gas)):
                out[f, rows, :] = now - scale * net[f]
        return tuple(out_carry)

    if first == 0:
        carry = tuple(jnp.zeros((8, lanes), jnp.float32) for _ in range(3 * chunks))
    else:
        carry = []
        for c in range(chunks):
            low, _, _ = load_state(press, depth, sat, at(first - 1, c))
            carry += flow_x(first - 1, c, low, None)
        carry = tuple(carry)
    end = min(last, cx - 1)
    carry = lax.fori_loop(first, end, lambda a, value: one_row(a, value, False), carry)
    if last == cx:
        one_row(cx - 1, carry, True)


def blocks_of(own, got_a, got_b, plus, minus):
    listing = [(own, 0), (got_a, 0), (got_b, 0)]
    listing += [(plus, b) for b in range(3)] + [(minus, b) for b in range(3)]
    return listing


def fault_kernel(
    own, got_a, got_b, plus, minus, press, depth, sat, _,
    back_plus, back_minus, back_y, local,
):
    listing = blocks_of(own, got_a, got_b, plus, minus)
    targets = [(back_y, k * FLOW) for k in range(3)]
    targets += [(back_plus, k * FLOW) for k in range(3)]
    targets += [(back_minus, k * FLOW) for k in range(3)]
    for n, (ref, block) in enumerate(listing):
        meta = ref[META + block : META + block + 1, :].astype(jnp.int32)
        for rank in range(CAP):
            col = meta[0, rank]
            at = n * 4 * CAP + rank
            local[at : at + 1, :] = press[pl.ds(col, 1), :]
            local[at + CAP : at + CAP + 1, :] = depth[pl.ds(col, 1), :]
            local[at + 2 * CAP : at + 2 * CAP + 1, :] = sat[0, pl.ds(col, 1), :]
            local[at + 3 * CAP : at + 3 * CAP + 1, :] = sat[1, pl.ds(col, 1), :]
    for n, (ref, block) in enumerate(listing):
        far = [ref[block * BLOCK + f * CAP : block * BLOCK + (f + 1) * CAP, :] for f in range(5)]
        near = [local[(n * 4 + f) * CAP : (n * 4 + f + 1) * CAP, :] for f in range(4)]
        flow = flux(
            (far[0], far[1]) + mobility(far[2], far[3]),
            (near[0], near[1]) + mobility(near[2], near[3]),
            far[4],
        )
        out, row = targets[n]
        for f in range(3):
            out[row + f * CAP : row + (f + 1) * CAP, :] = flow[f]
    for out in (back_plus, back_minus, back_y):
        out[3 * FLOW : BACK, :] = jnp.zeros((BACK - 3 * FLOW, out.shape[1]), jnp.float32)


def edge_kernel(
    nx, ny, cx, cy,
    own, got_a, got_b, plus, minus, back_plus, back_minus, back_y,
    hxa, hxb, hya, hyb, press, depth, sat, perm, pore, _,
    out,
):
    listing = blocks_of(own, got_a, got_b, plus, minus)
    sources = [(back_y, k * FLOW) for k in range(3)]
    sources += [(back_plus, k * FLOW) for k in range(3)]
    sources += [(back_minus, k * FLOW) for k in range(3)]
    home_x = lax.axis_index("gx")
    home_y = lax.axis_index("gy")
    columns = cx * cy

    def edge(first, second, count, dim, home, ends, rows_low, rows_high):
        even = lax.rem(home, 2) == 0
        for is_upper, rows in ((True, rows_high), (False, rows_low)):
            pick = even if is_upper else jnp.logical_not(even)
            far = [jnp.where(pick, first[f], second[f]) for f in range(5)]
            exists = (home < ends - 1) if is_upper else (home > 0)
            there = jnp.where(exists, 1.0, 0.0)
            mine, _, _ = load_state(press, depth, sat, rows)
            other = (far[0], far[1]) + mobility(far[2], far[3])
            trans = harmonic(perm[dim, rows, :], far[4]) * there
            if is_upper:
                flow = flux(mine, other, trans)
            else:
                flow = [-v for v in flux(other, mine, trans)]
            scale = STEP / pore[rows, :]
            for f in range(3):
                out[f, rows, :] = out[f, rows, :] - scale * flow[f]

    edge(hxa, hxb, cy, 0, home_x, nx, pl.ds(0, cy), pl.ds(columns - cy, cy))
    edge(hya, hyb, cx, 1, home_y, ny, pl.ds(0, cx, stride=cy), pl.ds(cy - 1, cx, stride=cy))
    for n, (ref, block) in enumerate(listing):
        meta = ref[META + block : META + block + 1, :].astype(jnp.int32)
        flows, row = sources[n]
        for rank in range(CAP):
            col = meta[0, rank]
            scale = STEP / pore[pl.ds(col, 1), :]
            for f in range(3):
                at = row + f * CAP + rank
                out[f, pl.ds(col, 1), :] = out[f, pl.ds(col, 1), :] + scale * flows[at : at + 1, :]


def finish_kernel(own, back_y, from_up, from_down, from_a, from_b, pore, _, out, work, sem):
    origin = own[META + 3 : META + 4, :].astype(jnp.int32)
    for ty in range(3):
        for tx in range(3):
            if ty > 0:
                ref, row = (from_a, from_b)[ty - 1], tx * FLOW
            elif tx == 0:
                ref, row = back_y, 0
            else:
                ref, row = (from_up, from_down)[tx - 1], 0
            for rank in range(CAP):
                col = origin[0, (ty * 3 + tx) * CAP + rank]
                scale = STEP / pore[pl.ds(col, 1), :]
                for f in range(3):
                    at = row + f * CAP + rank
                    work[f, pl.ds(col, 1), :] = (
                        work[f, pl.ds(col, 1), :] - scale * ref[at : at + 1, :]
                    )
    copy = pltpu.make_async_copy(work, out, sem)
    copy.start()
    copy.wait()


def swapped(value, axis, kind, other=None):
    count = lax.axis_size(axis)
    route = []
    for i in range(count):
        j = i ^ 1 if kind == 0 else (((i + 1) ^ 1) - 1) % count
        route.append((i, j))
    return lax.ppermute(value, axis, route)


def swapped_inside(value):
    nx, ny = lax.axis_size("gx"), lax.axis_size("gy")
    route = []
    for i in range(nx):
        for j in range(ny):
            if i in (0, nx - 1):
                route.append((i * ny + j, i * ny + (j ^ 1)))
            else:
                route.append((i * ny + j, (((i + 1) ^ 1) - 1) * ny + j))
    return lax.ppermute(value, ("gx", "gy"), route)


def shifted(value, axis, step):
    count = lax.axis_size(axis)
    return lax.ppermute(value, axis, [(i, (i + step) % count) for i in range(count)])


def relay_kernel(own, got_a, got_b, _, plus, minus):
    parts = (own, got_a, got_b)
    for tx, out in ((1, plus), (2, minus)):
        low = tx * BLOCK
        for k, part in enumerate(parts):
            out[k * BLOCK : (k + 1) * BLOCK, :] = part[low : low + BLOCK, :]
            out[META + k : META + k + 1, :] = part[META + tx : META + tx + 1, :]
        out[META + 3 :, :] = jnp.zeros((1, out.shape[1]), jnp.float32)


def relay_back_kernel(back_y, from_up, from_down, _, back_a, back_b):
    for ty, out in ((1, back_a), (2, back_b)):
        low = ty * FLOW
        for k, part in enumerate((back_y, from_up, from_down)):
            out[k * FLOW : (k + 1) * FLOW, :] = part[low : low + FLOW, :]
        out[3 * FLOW :, :] = jnp.zeros((BACK - 3 * FLOW, out.shape[1]), jnp.float32)


def body(
    pressure, depth, saturation, permeability, pore_volume,
    fault_pairs, fault_kind, fault_count, fault_table,
):
    cx, cy, layers = pressure.shape
    columns = cx * cy
    nx, ny = lax.axis_size("gx"), lax.axis_size("gy")
    f32 = jnp.float32
    slots = 9 * CAP
    rows = fault_pairs.shape[0]

    def flat(array):
        return array.reshape(array.shape[:-3] + (columns, layers))

    def cells(array):
        return array.reshape(array.shape[:-2] + (cx, cy, layers))

    def outer(array):
        return pltpu.with_memory_space_constraint(array, HBM)

    def vmem(*dims):
        return VMEM(dims, f32)

    message, back, full = vmem(ROWS, layers), vmem(BACK, layers), vmem(3, columns, layers)
    halo_x, halo_y = vmem(5, cy, layers), vmem(5, cx, layers)
    own, msg_a, msg_b, hxa, hxb, hya, hyb, press, deep, sat = pl.pallas_call(
        functools.partial(pack_kernel, nx, ny, cx, cy),
        in_specs=[spec(HBM)] * 11,
        out_specs=[spec(VMEM)] * 10,
        out_shape=[message] * 3 + [halo_x] * 2 + [halo_y] * 2
        + [vmem(columns, layers)] * 2 + [vmem(2, columns, layers)],
        scratch_shapes=[
            SMEM((3, rows), jnp.int32), SMEM((rows,), jnp.int32), SMEM((1, 1), jnp.int32),
            SMEM((nx * ny,), jnp.int32),
            SMEM((slots,), jnp.int32), SMEM((slots,), jnp.int32), SMEM((slots,), jnp.int32),
            SMEM((slots,), jnp.int32), SMEM((slots,), jnp.int32),
            VMEM(fault_table.shape, f32),
            pltpu.SemaphoreType.DMA((4,)), pltpu.SemaphoreType.DMA((3,)),
            pltpu.SemaphoreType.DMA((20,)),
        ],
        compiler_params=params(),
        cost_estimate=cost(4_000_000),
        name="pack",
    )(*map(lambda a: a if a.size <= 1 else outer(a), (
        fault_pairs.T, fault_kind, fault_count.reshape(1, 1), fault_table, pressure, depth, saturation,
        permeability, flat(pressure), flat(depth), flat(saturation),
    )))
    perm, pore = flat(permeability), flat(pore_volume)

    cuts = tuple(cx * k // 4 for k in range(5))

    def stencil(part, base):
        first, last = cuts[part], cuts[part + 1]
        operands = [press, deep, sat, perm, pore] + ([] if first == 0 else [base])
        return pl.pallas_call(
            functools.partial(stencil_kernel, cx, cy, first, last),
            in_specs=[spec(VMEM)] * 5 + ([] if first == 0 else [spec(pl.ANY)]),
            out_specs=spec(VMEM),
            out_shape=full,
            input_output_aliases={} if first == 0 else {5: 0},
            compiler_params=params(),
            cost_estimate=cost(8_000_000 * (last - first) // 8),
            name=f"stencil_{first}",
        )(*operands)

    got_a = swapped(msg_a, "gy", 0)
    got_b = swapped(msg_b, "gy", 1)
    base = stencil(0, None)
    plus, minus = pl.pallas_call(
        relay_kernel,
        in_specs=[spec(VMEM)] * 3 + [spec(pl.ANY)],
        out_specs=[spec(VMEM)] * 2,
        out_shape=[message] * 2,
        compiler_params=params(),
        cost_estimate=cost(100_000),
        name="relay",
    )(own, got_a, got_b, base)
    plus = shifted(plus, "gx", 1)
    minus = shifted(minus, "gx", -1)
    hxa, hxb = swapped(hxa, "gx", 0), swapped_inside(hxb)
    hya, hyb = swapped(hya, "gy", 0), swapped(hyb, "gy", 1)
    base = stencil(1, base)
    back_plus, back_minus, back_y = pl.pallas_call(
        fault_kernel,
        in_specs=[spec(VMEM)] * 8 + [spec(pl.ANY)],
        out_specs=[spec(VMEM)] * 3,
        out_shape=[back] * 3,
        scratch_shapes=[VMEM((slots * 4, layers), f32)],
        compiler_params=params(),
        cost_estimate=cost(2_000_000),
        name="fault",
    )(own, got_a, got_b, plus, minus, press, deep, sat, base)
    from_up = shifted(back_plus, "gx", -1)
    from_down = shifted(back_minus, "gx", 1)
    base = stencil(2, base)
    back_a, back_b = pl.pallas_call(
        relay_back_kernel,
        in_specs=[spec(VMEM)] * 3 + [spec(pl.ANY)],
        out_specs=[spec(VMEM)] * 2,
        out_shape=[back] * 2,
        compiler_params=params(),
        cost_estimate=cost(100_000),
        name="relay_back",
    )(back_y, from_up, from_down, base)
    from_a = swapped(back_a, "gy", 0)
    from_b = swapped(back_b, "gy", 1)
    base = stencil(3, base)
    base = pl.pallas_call(
        functools.partial(edge_kernel, nx, ny, cx, cy),
        in_specs=[spec(VMEM)] * 18,
        out_specs=spec(VMEM),
        out_shape=full,
        input_output_aliases={17: 0},
        compiler_params=params(),
        cost_estimate=cost(4_000_000),
        name="edge",
    )(own, got_a, got_b, plus, minus, back_plus, back_minus, back_y,
      hxa, hxb, hya, hyb, press, deep, sat, perm, pore, base)
    out, _ = pl.pallas_call(
        finish_kernel,
        in_specs=[spec(VMEM)] * 8,
        out_specs=[spec(HBM), spec(VMEM)],
        out_shape=[jax.ShapeDtypeStruct((3, columns, layers), f32), full],
        input_output_aliases={7: 1},
        scratch_shapes=[pltpu.SemaphoreType.DMA],
        compiler_params=params(),
        cost_estimate=cost(2_000_000),
        name="finish",
    )(own, back_y, from_up, from_down, from_a, from_b, pore, base)
    return cells(out)


def solution(mesh):
    in_specs = (
        P("gx", "gy", None),
        P("gx", "gy", None),
        P(None, "gx", "gy", None),
        P(None, "gx", "gy", None),
        P("gx", "gy", None),
        P(("gx", "gy"), None),
        P(("gx", "gy")),
        P(("gx", "gy")),
        P(),
    )
    out_specs = P(None, "gx", "gy", None)
    return jax.shard_map(body, mesh=mesh, in_specs=in_specs, out_specs=out_specs, check_vma=False)
```

```python
import functools

import jax
import jax.numpy as jnp
from jax import lax
from jax.experimental import pallas as pl
from jax.experimental.pallas import tpu as pltpu
from jax.sharding import PartitionSpec as P


CAP = 4
FIELDS = 5
BLOCK = CAP * FIELDS
META = 3 * BLOCK
ROWS = 64
FLOW = 3 * CAP
BACK = 40

VISCOSITY = (0.5, 1.0, 0.25)
DENSITY = (1.0, 0.8, 0.25)
STEP = 0.2


VMEM = pltpu.VMEM
HBM = pltpu.HBM
SMEM = pltpu.SMEM


def spec(space):
    return pl.BlockSpec(memory_space=space)


def params(limit=6):
    return pltpu.CompilerParams(vmem_limit_bytes=limit * 2**20)


def cost(flops):
    return pl.CostEstimate(flops=flops, bytes_accessed=flops // 64, transcendentals=0)


def mobility(water, oil):
    gas = 1.0 - water - oil
    return (
        water * water * (1.0 / VISCOSITY[0]),
        oil * oil * (1.0 / VISCOSITY[1]),
        gas * gas * (1.0 / VISCOSITY[2]),
    )


def harmonic(first, second):
    return (first * second + first * second) / (first + second)


def flux(low, high, trans):
    dp = low[0] - high[0]
    dd = low[1] - high[1]
    flows = []
    for phase in range(3):
        drive = dp - DENSITY[phase] * dd if DENSITY[phase] != 1.0 else dp - dd
        up = jnp.where(drive > 0.0, low[2 + phase], high[2 + phase])
        flows.append(trans * drive * up)
    return flows


def pack_kernel(
    nx, ny,
    pairs_ref, kind_ref, count_ref, table_ref, press_f, depth_f, sat_f,
    own, msg_a, msg_b, press, depth, sat,
    pairs_s, kind_s, count_s, slot_s, seen_s, src_s, knd_s, liv_s, lnd_s, table,
    sem_i, sem_s,
):
    ints = [
        pltpu.make_async_copy(pairs_ref, pairs_s, sem_i.at[0]),
        pltpu.make_async_copy(kind_ref, kind_s, sem_i.at[1]),
        pltpu.make_async_copy(count_ref, count_s, sem_i.at[2]),
        pltpu.make_async_copy(table_ref, table, sem_i.at[3]),
    ]
    for copy in ints:
        copy.start()
    bulk = [
        pltpu.make_async_copy(press_f, press, sem_s.at[0]),
        pltpu.make_async_copy(depth_f, depth, sem_s.at[1]),
        pltpu.make_async_copy(sat_f, sat, sem_s.at[2]),
    ]
    for copy in bulk:
        copy.start()
    home_x = lax.axis_index("gx")
    home_y = lax.axis_index("gy")
    even_y = lax.rem(home_y, 2) == 0
    for step_x in (0, 1, -1):
        to_x = lax.rem(home_x + step_x + nx, nx)
        tx = step_x % 3
        for step_y in (0, 1, -1):
            to_y = lax.rem(home_y + step_y + ny, ny)
            if step_y == 0:
                ty = 0
            else:
                ty = jnp.where(even_y == (step_y == 1), 1, 2)
            slot_s[to_x * ny + to_y] = (ty * 3 + tx) * CAP
    for k in range(9 * CAP):
        seen_s[k] = 0
        src_s[k] = 0
        knd_s[k] = 0
        liv_s[k] = 0
        lnd_s[k] = 0
    for copy in ints:
        copy.wait()
    count = count_s[0, 0]
    for r in range(pairs_s.shape[1]):
        base = slot_s[pairs_s[1, r]]
        rank = seen_s[base]
        seen_s[base] = rank + 1
        position = base + rank
        src_s[position] = pairs_s[0, r]
        lnd_s[position] = pairs_s[2, r]
        knd_s[position] = kind_s[r]
        liv_s[position] = jnp.where(r < count, 1, 0)
    lane = lax.broadcasted_iota(jnp.int32, (1, own.shape[1]), 1)
    messages = (own, msg_a, msg_b)
    origin = jnp.zeros(lane.shape, jnp.int32)
    for ty in range(3):
        out = messages[ty]
        for tx in range(3):
            meta = jnp.zeros(lane.shape, jnp.int32)
            for rank in range(CAP):
                k = (ty * 3 + tx) * CAP + rank
                meta = jnp.where(lane == rank, lnd_s[k], meta)
                origin = jnp.where(lane == k, src_s[k], origin)
                trans = table[pl.ds(knd_s[k], 1), :]
                alive = liv_s[k].astype(jnp.float32)
                out[tx * BLOCK + 4 * CAP + rank : tx * BLOCK + 4 * CAP + rank + 1, :] = trans * alive
            out[META + tx : META + tx + 1, :] = meta.astype(jnp.float32)
        out[META + 3 : META + 4, :] = jnp.zeros(lane.shape, jnp.float32)
    own[META + 3 : META + 4, :] = origin.astype(jnp.float32)
    for copy in bulk:
        copy.wait()
    for ty in range(3):
        out = messages[ty]
        for tx in range(3):
            for rank in range(CAP):
                k = (ty * 3 + tx) * CAP + rank
                col = src_s[k]
                at = tx * BLOCK + rank
                out[at : at + 1, :] = press[pl.ds(col, 1), :]
                out[at + CAP : at + CAP + 1, :] = depth[pl.ds(col, 1), :]
                out[at + 2 * CAP : at + 2 * CAP + 1, :] = sat[0, pl.ds(col, 1), :]
                out[at + 3 * CAP : at + 3 * CAP + 1, :] = sat[1, pl.ds(col, 1), :]


def load_state(press, depth, sat, rows):
    water, oil = sat[0, rows, :], sat[1, rows, :]
    return (press[rows, :], depth[rows, :]) + mobility(water, oil), water, oil


def stencil_kernel(cx, cy, first, last, *refs):
    if first == 0:
        press, depth, sat, perm, pore, out = refs
    else:
        press, depth, sat, perm, pore, _, out = refs
    lanes = press.shape[1]
    lane = lax.broadcasted_iota(jnp.int32, (8, lanes), 1)
    sub = lax.broadcasted_iota(jnp.int32, (8, lanes), 0)
    chunks = cy // 8

    def at(a, c, shift=0):
        return pl.ds(pl.multiple_of(a * cy, 8) + (c * 8 + shift), 8)

    def flow_x(a, c, low):
        rows = at(a + 1, c)
        high, _, _ = load_state(press, depth, sat, rows)
        trans = harmonic(perm[0, at(a, c), :], perm[0, rows, :])
        return flux(low, high, trans)

    def one_row(a, carry, top):
        out_carry = []
        below = None
        for c in range(chunks):
            rows = at(a, c)
            mine, water, oil = load_state(press, depth, sat, rows)
            if top:
                net = [-carry[3 * c + f] for f in range(3)]
            else:
                up = flow_x(a, c, mine)
                out_carry += up
                net = [up[f] - carry[3 * c + f] for f in range(3)]
            ky = perm[1, rows, :]
            if c < chunks - 1:
                rows_up = at(a, c, 1)
                high, _, _ = load_state(press, depth, sat, rows_up)
                trans = harmonic(ky, perm[1, rows_up, :])
            else:
                high = tuple(pltpu.roll(v, 7, 0) for v in mine)
                trans = jnp.where(sub < 7, harmonic(ky, pltpu.roll(ky, 7, 0)), 0.0)
            flow = flux(mine, high, trans)
            for f in range(3):
                back = pltpu.roll(flow[f], 1, 0)
                first_row = jnp.zeros_like(back) if c == 0 else below[f]
                net[f] = net[f] + (flow[f] - jnp.where(sub == 0, first_row, back))
            below = [pltpu.roll(flow[f], 1, 0) for f in range(3)]
            kz = perm[2, rows, :]
            high = tuple(pltpu.roll(v, lanes - 1, 1) for v in mine)
            trans = jnp.where(lane < lanes - 1, harmonic(kz, pltpu.roll(kz, lanes - 1, 1)), 0.0)
            flow = flux(mine, high, trans)
            for f in range(3):
                net[f] = net[f] + (flow[f] - pltpu.roll(flow[f], 1, 1))
            scale = STEP / pore[rows, :]
            gas = 1.0 - water - oil
            for f, now in enumerate((water, oil, gas)):
                out[f, rows, :] = now - scale * net[f]
        return tuple(out_carry)

    if first == 0:
        carry = tuple(jnp.zeros((8, lanes), jnp.float32) for _ in range(3 * chunks))
    else:
        carry = []
        for c in range(chunks):
            low, _, _ = load_state(press, depth, sat, at(first - 1, c))
            carry += flow_x(first - 1, c, low)
        carry = tuple(carry)
    end = min(last, cx - 1)
    carry = lax.fori_loop(first, end, lambda a, value: one_row(a, value, False), carry)
    if last == cx:
        one_row(cx - 1, carry, True)


def halo_kernel(cx, cy, press, depth, sat, perm, _, hxa, hxb, hya, hyb):
    even_x = lax.rem(lax.axis_index("gx"), 2) == 0
    even_y = lax.rem(lax.axis_index("gy"), 2) == 0
    columns = cx * cy
    low, high = pl.ds(0, cy), pl.ds(columns - cy, cy)
    left, right = pl.ds(0, cx, stride=cy), pl.ds(cy - 1, cx, stride=cy)
    for field in range(5):

        def rows(where, dim):
            if field < 2:
                return (press, depth)[field][where, :]
            return sat[field - 2, where, :] if field < 4 else perm[dim, where, :]

        first, last = rows(low, 0), rows(high, 0)
        hxa[field] = jnp.where(even_x, last, first)
        hxb[field] = jnp.where(even_x, first, last)
        first, last = rows(left, 1), rows(right, 1)
        hya[field] = jnp.where(even_y, last, first)
        hyb[field] = jnp.where(even_y, first, last)


def blocks_of(own, got_a, got_b, plus, minus):
    listing = [(own, 0), (got_a, 0), (got_b, 0)]
    listing += [(plus, b) for b in range(3)] + [(minus, b) for b in range(3)]
    return listing


def fault_kernel(
    own, got_a, got_b, plus, minus, press, depth, sat, _,
    back_plus, back_minus, back_y, local,
):
    listing = blocks_of(own, got_a, got_b, plus, minus)
    targets = [(back_y, k * FLOW) for k in range(3)]
    targets += [(back_plus, k * FLOW) for k in range(3)]
    targets += [(back_minus, k * FLOW) for k in range(3)]
    for n, (ref, block) in enumerate(listing):
        meta = ref[META + block : META + block + 1, :].astype(jnp.int32)
        for rank in range(CAP):
            col = meta[0, rank]
            at = n * 4 * CAP + rank
            local[at : at + 1, :] = press[pl.ds(col, 1), :]
            local[at + CAP : at + CAP + 1, :] = depth[pl.ds(col, 1), :]
            local[at + 2 * CAP : at + 2 * CAP + 1, :] = sat[0, pl.ds(col, 1), :]
            local[at + 3 * CAP : at + 3 * CAP + 1, :] = sat[1, pl.ds(col, 1), :]
    for n, (ref, block) in enumerate(listing):
        far = [ref[block * BLOCK + f * CAP : block * BLOCK + (f + 1) * CAP, :] for f in range(5)]
        near = [local[(n * 4 + f) * CAP : (n * 4 + f + 1) * CAP, :] for f in range(4)]
        flow = flux(
            (far[0], far[1]) + mobility(far[2], far[3]),
            (near[0], near[1]) + mobility(near[2], near[3]),
            far[4],
        )
        out, row = targets[n]
        for f in range(3):
            out[row + f * CAP : row + (f + 1) * CAP, :] = flow[f]
    for out in (back_plus, back_minus, back_y):
        out[3 * FLOW : BACK, :] = jnp.zeros((BACK - 3 * FLOW, out.shape[1]), jnp.float32)


def edge_kernel(
    nx, ny, cx, cy,
    own, got_a, got_b, plus, minus, back_plus, back_minus, back_y,
    hxa, hxb, hya, hyb, press, depth, sat, perm, pore, _,
    out,
):
    listing = blocks_of(own, got_a, got_b, plus, minus)
    sources = [(back_y, k * FLOW) for k in range(3)]
    sources += [(back_plus, k * FLOW) for k in range(3)]
    sources += [(back_minus, k * FLOW) for k in range(3)]
    home_x = lax.axis_index("gx")
    home_y = lax.axis_index("gy")
    columns = cx * cy

    def edge(first, second, dim, home, ends, rows_low, rows_high):
        even = lax.rem(home, 2) == 0
        for is_upper, rows in ((True, rows_high), (False, rows_low)):
            pick = even if is_upper else jnp.logical_not(even)
            far = [jnp.where(pick, first[f], second[f]) for f in range(5)]
            exists = (home < ends - 1) if is_upper else (home > 0)
            there = jnp.where(exists, 1.0, 0.0)
            mine, _, _ = load_state(press, depth, sat, rows)
            other = (far[0], far[1]) + mobility(far[2], far[3])
            trans = harmonic(perm[dim, rows, :], far[4]) * there
            if is_upper:
                flow = flux(mine, other, trans)
            else:
                flow = [-v for v in flux(other, mine, trans)]
            scale = STEP / pore[rows, :]
            for f in range(3):
                out[f, rows, :] = out[f, rows, :] - scale * flow[f]

    edge(hxa, hxb, 0, home_x, nx, pl.ds(0, cy), pl.ds(columns - cy, cy))
    edge(hya, hyb, 1, home_y, ny, pl.ds(0, cx, stride=cy), pl.ds(cy - 1, cx, stride=cy))
    for n, (ref, block) in enumerate(listing):
        meta = ref[META + block : META + block + 1, :].astype(jnp.int32)
        flows, row = sources[n]
        for rank in range(CAP):
            col = meta[0, rank]
            scale = STEP / pore[pl.ds(col, 1), :]
            for f in range(3):
                at = row + f * CAP + rank
                out[f, pl.ds(col, 1), :] = out[f, pl.ds(col, 1), :] + scale * flows[at : at + 1, :]


def finish_kernel(own, back_y, from_up, from_down, from_a, from_b, pore, _, out, work, sem):
    origin = own[META + 3 : META + 4, :].astype(jnp.int32)
    for ty in range(3):
        for tx in range(3):
            if ty > 0:
                ref, row = (from_a, from_b)[ty - 1], tx * FLOW
            elif tx == 0:
                ref, row = back_y, 0
            else:
                ref, row = (from_up, from_down)[tx - 1], 0
            for rank in range(CAP):
                col = origin[0, (ty * 3 + tx) * CAP + rank]
                scale = STEP / pore[pl.ds(col, 1), :]
                for f in range(3):
                    at = row + f * CAP + rank
                    work[f, pl.ds(col, 1), :] = (
                        work[f, pl.ds(col, 1), :] - scale * ref[at : at + 1, :]
                    )
    copy = pltpu.make_async_copy(work, out, sem)
    copy.start()
    copy.wait()


def swapped(value, axis, kind):
    count = lax.axis_size(axis)
    route = []
    for i in range(count):
        j = i ^ 1 if kind == 0 else (((i + 1) ^ 1) - 1) % count
        route.append((i, j))
    return lax.ppermute(value, axis, route)


def swapped_inside(value):
    nx, ny = lax.axis_size("gx"), lax.axis_size("gy")
    route = []
    for i in range(nx):
        for j in range(ny):
            if i in (0, nx - 1):
                route.append((i * ny + j, i * ny + (j ^ 1)))
            else:
                route.append((i * ny + j, (((i + 1) ^ 1) - 1) * ny + j))
    return lax.ppermute(value, ("gx", "gy"), route)


def shifted(value, axis, step):
    count = lax.axis_size(axis)
    return lax.ppermute(value, axis, [(i, (i + step) % count) for i in range(count)])


def relay_kernel(own, got_a, got_b, _, plus, minus):
    parts = (own, got_a, got_b)
    for tx, out in ((1, plus), (2, minus)):
        low = tx * BLOCK
        for k, part in enumerate(parts):
            out[k * BLOCK : (k + 1) * BLOCK, :] = part[low : low + BLOCK, :]
            out[META + k : META + k + 1, :] = part[META + tx : META + tx + 1, :]
        out[META + 3 :, :] = jnp.zeros((1, out.shape[1]), jnp.float32)


def relay_back_kernel(back_y, from_up, from_down, _, back_a, back_b):
    for ty, out in ((1, back_a), (2, back_b)):
        low = ty * FLOW
        for k, part in enumerate((back_y, from_up, from_down)):
            out[k * FLOW : (k + 1) * FLOW, :] = part[low : low + FLOW, :]
        out[3 * FLOW :, :] = jnp.zeros((BACK - 3 * FLOW, out.shape[1]), jnp.float32)


def step(
    pressure, depth, saturation, permeability, pore_volume,
    fault_pairs, fault_kind, fault_count, fault_table,
):
    cx, cy, layers = pressure.shape
    columns = cx * cy
    nx, ny = lax.axis_size("gx"), lax.axis_size("gy")
    f32 = jnp.float32
    slots = 9 * CAP
    rows = fault_pairs.shape[0]

    def flat(array):
        return array.reshape(array.shape[:-3] + (columns, layers))

    def cells(array):
        return array.reshape(array.shape[:-2] + (cx, cy, layers))

    def outer(array):
        return pltpu.with_memory_space_constraint(array, HBM)

    def vmem(*dims):
        return VMEM(dims, f32)

    message, back, full = vmem(ROWS, layers), vmem(BACK, layers), vmem(3, columns, layers)
    halo_x, halo_y = vmem(5, cy, layers), vmem(5, cx, layers)
    own, msg_a, msg_b, press, deep, sat = pl.pallas_call(
        functools.partial(pack_kernel, nx, ny),
        in_specs=[spec(HBM)] * 7,
        out_specs=[spec(VMEM)] * 6,
        out_shape=[message] * 3
        + [vmem(columns, layers)] * 2 + [vmem(2, columns, layers)],
        scratch_shapes=[
            SMEM((3, rows), jnp.int32), SMEM((rows,), jnp.int32), SMEM((1, 1), jnp.int32),
            SMEM((nx * ny,), jnp.int32),
            SMEM((slots,), jnp.int32), SMEM((slots,), jnp.int32), SMEM((slots,), jnp.int32),
            SMEM((slots,), jnp.int32), SMEM((slots,), jnp.int32),
            VMEM(fault_table.shape, f32),
            pltpu.SemaphoreType.DMA((4,)), pltpu.SemaphoreType.DMA((3,)),
        ],
        compiler_params=params(),
        cost_estimate=cost(4_000_000),
        name="pack",
    )(*map(lambda a: a if a.size <= 1 else outer(a), (
        fault_pairs.T, fault_kind, fault_count.reshape(1, 1), fault_table,
        flat(pressure), flat(depth), flat(saturation),
    )))
    perm, pore = flat(permeability), flat(pore_volume)

    cuts = tuple(cx * k // 4 for k in range(5))

    def stencil(part, base):
        first, last = cuts[part], cuts[part + 1]
        operands = [press, deep, sat, perm, pore] + ([] if first == 0 else [base])
        return pl.pallas_call(
            functools.partial(stencil_kernel, cx, cy, first, last),
            in_specs=[spec(VMEM)] * 5 + ([] if first == 0 else [spec(pl.ANY)]),
            out_specs=spec(VMEM),
            out_shape=full,
            input_output_aliases={} if first == 0 else {5: 0},
            compiler_params=params(),
            cost_estimate=cost(8_000_000 * (last - first) // 8),
        )(*operands)

    got_a = swapped(msg_a, "gy", 0)
    got_b = swapped(msg_b, "gy", 1)
    base = stencil(0, None)
    plus, minus = pl.pallas_call(
        relay_kernel,
        in_specs=[spec(VMEM)] * 3 + [spec(pl.ANY)],
        out_specs=[spec(VMEM)] * 2,
        out_shape=[message] * 2,
        compiler_params=params(),
        cost_estimate=cost(100_000),
        name="relay",
    )(own, got_a, got_b, base)
    plus = shifted(plus, "gx", 1)
    minus = shifted(minus, "gx", -1)
    base = stencil(1, base)
    back_plus, back_minus, back_y = pl.pallas_call(
        fault_kernel,
        in_specs=[spec(VMEM)] * 8 + [spec(pl.ANY)],
        out_specs=[spec(VMEM)] * 3,
        out_shape=[back] * 3,
        scratch_shapes=[VMEM((slots * 4, layers), f32)],
        compiler_params=params(),
        cost_estimate=cost(2_000_000),
        name="fault",
    )(own, got_a, got_b, plus, minus, press, deep, sat, base)
    from_down = shifted(back_minus, "gx", 1)
    from_up = shifted(back_plus, "gx", -1)
    hxa, hxb, hya, hyb = pl.pallas_call(
        functools.partial(halo_kernel, cx, cy),
        in_specs=[spec(VMEM)] * 4 + [spec(pl.ANY)],
        out_specs=[spec(VMEM)] * 4,
        out_shape=[halo_x] * 2 + [halo_y] * 2,
        compiler_params=params(),
        cost_estimate=cost(100_000),
        name="halo",
    )(press, deep, sat, perm, back_y)
    hxa = swapped(hxa, "gx", 0)
    hxb = swapped_inside(hxb)
    hya = swapped(hya, "gy", 0)
    hyb = swapped(hyb, "gy", 1)
    base = stencil(2, base)
    back_a, back_b = pl.pallas_call(
        relay_back_kernel,
        in_specs=[spec(VMEM)] * 3 + [spec(pl.ANY)],
        out_specs=[spec(VMEM)] * 2,
        out_shape=[back] * 2,
        compiler_params=params(),
        cost_estimate=cost(100_000),
        name="relay_back",
    )(back_y, from_up, from_down, base)
    from_a = swapped(back_a, "gy", 0)
    from_b = swapped(back_b, "gy", 1)
    base = stencil(3, base)
    base = pl.pallas_call(
        functools.partial(edge_kernel, nx, ny, cx, cy),
        in_specs=[spec(VMEM)] * 18,
        out_specs=spec(VMEM),
        out_shape=full,
        input_output_aliases={17: 0},
        compiler_params=params(),
        cost_estimate=cost(4_000_000),
        name="edge",
    )(own, got_a, got_b, plus, minus, back_plus, back_minus, back_y,
      hxa, hxb, hya, hyb, press, deep, sat, perm, pore, base)
    out, _ = pl.pallas_call(
        finish_kernel,
        in_specs=[spec(VMEM)] * 8,
        out_specs=[spec(HBM), spec(VMEM)],
        out_shape=[jax.ShapeDtypeStruct((3, columns, layers), f32), full],
        input_output_aliases={7: 1},
        scratch_shapes=[pltpu.SemaphoreType.DMA],
        compiler_params=params(),
        cost_estimate=cost(2_000_000),
        name="finish",
    )(own, back_y, from_up, from_down, from_a, from_b, pore, base)
    return cells(out)


def solution(mesh):
    in_specs = (
        P("gx", "gy", None),
        P("gx", "gy", None),
        P(None, "gx", "gy", None),
        P(None, "gx", "gy", None),
        P("gx", "gy", None),
        P(("gx", "gy"), None),
        P(("gx", "gy")),
        P(("gx", "gy")),
        P(),
    )
    out_specs = P(None, "gx", "gy", None)
    return jax.shard_map(step, mesh=mesh, in_specs=in_specs, out_specs=out_specs, check_vma=False)
```

```python
import functools

import jax
import jax.numpy as jnp
from jax import lax
from jax.experimental import pallas as pl
from jax.experimental.pallas import tpu as pltpu
from jax.sharding import PartitionSpec as P


CAP = 4
FIELDS = 5
BLOCK = CAP * FIELDS
META = 3 * BLOCK
ROWS = 64
FLOW = 3 * CAP
BACK = 40

VISCOSITY = (0.5, 1.0, 0.25)
DENSITY = (1.0, 0.8, 0.25)
STEP = 0.2


VMEM = pltpu.VMEM
HBM = pltpu.HBM
SMEM = pltpu.SMEM


def spec(space):
    return pl.BlockSpec(memory_space=space)


def params(limit=6):
    return pltpu.CompilerParams(vmem_limit_bytes=limit * 2**20)


def cost(flops):
    return pl.CostEstimate(flops=flops, bytes_accessed=flops // 64, transcendentals=0)


def mobility(water, oil):
    gas = 1.0 - water - oil
    return (
        water * water * (1.0 / VISCOSITY[0]),
        oil * oil * (1.0 / VISCOSITY[1]),
        gas * gas * (1.0 / VISCOSITY[2]),
    )


def harmonic(first, second):
    return (first * second + first * second) / (first + second)


def flux(low, high, trans):
    dp = low[0] - high[0]
    dd = low[1] - high[1]
    flows = []
    for phase in range(3):
        drive = dp - DENSITY[phase] * dd if DENSITY[phase] != 1.0 else dp - dd
        up = jnp.where(drive > 0.0, low[2 + phase], high[2 + phase])
        flows.append(trans * drive * up)
    return flows


def pack_kernel(
    nx, ny,
    pairs_ref, kind_ref, count_ref, table_ref, press_f, depth_f, sat_f,
    own, msg_a, msg_b, press, depth, sat,
    pairs_s, kind_s, count_s, slot_s, seen_s, src_s, knd_s, liv_s, lnd_s, table,
    sem_i, sem_s,
):
    ints = [
        pltpu.make_async_copy(pairs_ref, pairs_s, sem_i.at[0]),
        pltpu.make_async_copy(kind_ref, kind_s, sem_i.at[1]),
        pltpu.make_async_copy(count_ref, count_s, sem_i.at[2]),
        pltpu.make_async_copy(table_ref, table, sem_i.at[3]),
    ]
    for copy in ints:
        copy.start()
    bulk = [
        pltpu.make_async_copy(press_f, press, sem_s.at[0]),
        pltpu.make_async_copy(depth_f, depth, sem_s.at[1]),
        pltpu.make_async_copy(sat_f, sat, sem_s.at[2]),
    ]
    for copy in bulk:
        copy.start()
    home_x = lax.axis_index("gx")
    home_y = lax.axis_index("gy")
    even_y = lax.rem(home_y, 2) == 0
    for step_x in (0, 1, -1):
        to_x = lax.rem(home_x + step_x + nx, nx)
        tx = step_x % 3
        for step_y in (0, 1, -1):
            to_y = lax.rem(home_y + step_y + ny, ny)
            if step_y == 0:
                ty = 0
            else:
                ty = jnp.where(even_y == (step_y == 1), 1, 2)
            slot_s[to_x * ny + to_y] = (ty * 3 + tx) * CAP
    for k in range(9 * CAP):
        seen_s[k] = 0
        src_s[k] = 0
        knd_s[k] = 0
        liv_s[k] = 0
        lnd_s[k] = 0
    for copy in ints:
        copy.wait()
    count = count_s[0, 0]
    for r in range(pairs_s.shape[1]):
        base = slot_s[pairs_s[1, r]]
        rank = seen_s[base]
        seen_s[base] = rank + 1
        position = base + rank
        src_s[position] = pairs_s[0, r]
        lnd_s[position] = pairs_s[2, r]
        knd_s[position] = kind_s[r]
        liv_s[position] = jnp.where(r < count, 1, 0)
    lane = lax.broadcasted_iota(jnp.int32, (1, own.shape[1]), 1)
    messages = (own, msg_a, msg_b)
    origin = jnp.zeros(lane.shape, jnp.int32)
    for ty in range(3):
        out = messages[ty]
        for tx in range(3):
            meta = jnp.zeros(lane.shape, jnp.int32)
            for rank in range(CAP):
                k = (ty * 3 + tx) * CAP + rank
                meta = jnp.where(lane == rank, lnd_s[k], meta)
                origin = jnp.where(lane == k, src_s[k], origin)
                trans = table[pl.ds(knd_s[k], 1), :]
                alive = liv_s[k].astype(jnp.float32)
                out[tx * BLOCK + 4 * CAP + rank : tx * BLOCK + 4 * CAP + rank + 1, :] = trans * alive
            out[META + tx : META + tx + 1, :] = meta.astype(jnp.float32)
        out[META + 3 : META + 4, :] = jnp.zeros(lane.shape, jnp.float32)
    own[META + 3 : META + 4, :] = origin.astype(jnp.float32)
    for copy in bulk:
        copy.wait()
    for ty in range(3):
        out = messages[ty]
        for tx in range(3):
            for rank in range(CAP):
                k = (ty * 3 + tx) * CAP + rank
                col = src_s[k]
                at = tx * BLOCK + rank
                out[at : at + 1, :] = press[pl.ds(col, 1), :]
                out[at + CAP : at + CAP + 1, :] = depth[pl.ds(col, 1), :]
                out[at + 2 * CAP : at + 2 * CAP + 1, :] = sat[0, pl.ds(col, 1), :]
                out[at + 3 * CAP : at + 3 * CAP + 1, :] = sat[1, pl.ds(col, 1), :]


def load_state(press, depth, sat, rows):
    water, oil = sat[0, rows, :], sat[1, rows, :]
    return (press[rows, :], depth[rows, :]) + mobility(water, oil), water, oil


def chosen(role):
    if role is None:
        return True
    return (lax.axis_index("gx") == 0) == role


def stencil_kernel(cx, cy, first, last, role, *refs):
    @pl.when(chosen(role))
    def _():
        stencil_rows(cx, cy, first, last, *refs)


def stencil_rows(cx, cy, first, last, *refs):
    press, depth, sat, perm, pore = refs[:5]
    out = refs[-1]
    lanes = press.shape[1]
    lane = lax.broadcasted_iota(jnp.int32, (8, lanes), 1)
    sub = lax.broadcasted_iota(jnp.int32, (8, lanes), 0)
    chunks = cy // 8

    def at(a, c, shift=0):
        return pl.ds(pl.multiple_of(a * cy, 8) + (c * 8 + shift), 8)

    def flow_x(a, c, low):
        rows = at(a + 1, c)
        high, _, _ = load_state(press, depth, sat, rows)
        trans = harmonic(perm[0, at(a, c), :], perm[0, rows, :])
        return flux(low, high, trans)

    def one_row(a, carry, top):
        out_carry = []
        below = None
        for c in range(chunks):
            rows = at(a, c)
            mine, water, oil = load_state(press, depth, sat, rows)
            if top:
                net = [-carry[3 * c + f] for f in range(3)]
            else:
                up = flow_x(a, c, mine)
                out_carry += up
                net = [up[f] - carry[3 * c + f] for f in range(3)]
            ky = perm[1, rows, :]
            if c < chunks - 1:
                rows_up = at(a, c, 1)
                high, _, _ = load_state(press, depth, sat, rows_up)
                trans = harmonic(ky, perm[1, rows_up, :])
            else:
                high = tuple(pltpu.roll(v, 7, 0) for v in mine)
                trans = jnp.where(sub < 7, harmonic(ky, pltpu.roll(ky, 7, 0)), 0.0)
            flow = flux(mine, high, trans)
            for f in range(3):
                back = pltpu.roll(flow[f], 1, 0)
                first_row = jnp.zeros_like(back) if c == 0 else below[f]
                net[f] = net[f] + (flow[f] - jnp.where(sub == 0, first_row, back))
            below = [pltpu.roll(flow[f], 1, 0) for f in range(3)]
            kz = perm[2, rows, :]
            high = tuple(pltpu.roll(v, lanes - 1, 1) for v in mine)
            trans = jnp.where(lane < lanes - 1, harmonic(kz, pltpu.roll(kz, lanes - 1, 1)), 0.0)
            flow = flux(mine, high, trans)
            for f in range(3):
                net[f] = net[f] + (flow[f] - pltpu.roll(flow[f], 1, 1))
            scale = STEP / pore[rows, :]
            gas = 1.0 - water - oil
            for f, now in enumerate((water, oil, gas)):
                out[f, rows, :] = now - scale * net[f]
        return tuple(out_carry)

    if first == 0:
        carry = tuple(jnp.zeros((8, lanes), jnp.float32) for _ in range(3 * chunks))
    else:
        carry = []
        for c in range(chunks):
            low, _, _ = load_state(press, depth, sat, at(first - 1, c))
            carry += flow_x(first - 1, c, low)
        carry = tuple(carry)
    end = min(last, cx - 1)
    carry = lax.fori_loop(first, end, lambda a, value: one_row(a, value, False), carry, unroll=2)
    if last == cx:
        one_row(cx - 1, carry, True)


def halo_kernel(cx, cy, press, depth, sat, perm, hxa, hxb, hya, hyb):
    even_x = lax.rem(lax.axis_index("gx"), 2) == 0
    even_y = lax.rem(lax.axis_index("gy"), 2) == 0
    columns = cx * cy
    low, high = pl.ds(0, cy), pl.ds(columns - cy, cy)
    left, right = pl.ds(0, cx, stride=cy), pl.ds(cy - 1, cx, stride=cy)
    for field in range(5):

        def rows(where, dim):
            if field < 2:
                return (press, depth)[field][where, :]
            return sat[field - 2, where, :] if field < 4 else perm[dim, where, :]

        first, last = rows(low, 0), rows(high, 0)
        hxa[field] = jnp.where(even_x, last, first)
        hxb[field] = jnp.where(even_x, first, last)
        first, last = rows(left, 1), rows(right, 1)
        hya[field] = jnp.where(even_y, last, first)
        hyb[field] = jnp.where(even_y, first, last)


def blocks_of(own, got_a, got_b, plus, minus):
    listing = [(own, 0), (got_a, 0), (got_b, 0)]
    listing += [(plus, b) for b in range(3)] + [(minus, b) for b in range(3)]
    return listing


def fault_kernel(
    own, got_a, got_b, plus, minus, press, depth, sat, _,
    back_plus, back_minus, back_y, local,
):
    listing = blocks_of(own, got_a, got_b, plus, minus)
    targets = [(back_y, k * FLOW) for k in range(3)]
    targets += [(back_plus, k * FLOW) for k in range(3)]
    targets += [(back_minus, k * FLOW) for k in range(3)]
    for n, (ref, block) in enumerate(listing):
        meta = ref[META + block : META + block + 1, :].astype(jnp.int32)
        for rank in range(CAP):
            col = meta[0, rank]
            at = n * 4 * CAP + rank
            local[at : at + 1, :] = press[pl.ds(col, 1), :]
            local[at + CAP : at + CAP + 1, :] = depth[pl.ds(col, 1), :]
            local[at + 2 * CAP : at + 2 * CAP + 1, :] = sat[0, pl.ds(col, 1), :]
            local[at + 3 * CAP : at + 3 * CAP + 1, :] = sat[1, pl.ds(col, 1), :]
    for n, (ref, block) in enumerate(listing):
        far = [ref[block * BLOCK + f * CAP : block * BLOCK + (f + 1) * CAP, :] for f in range(5)]
        near = [local[(n * 4 + f) * CAP : (n * 4 + f + 1) * CAP, :] for f in range(4)]
        flow = flux(
            (far[0], far[1]) + mobility(far[2], far[3]),
            (near[0], near[1]) + mobility(near[2], near[3]),
            far[4],
        )
        out, row = targets[n]
        for f in range(3):
            out[row + f * CAP : row + (f + 1) * CAP, :] = flow[f]
    for out in (back_plus, back_minus, back_y):
        out[3 * FLOW : BACK, :] = jnp.zeros((BACK - 3 * FLOW, out.shape[1]), jnp.float32)


def edge_kernel(nx, ny, cx, cy, role, *refs):
    @pl.when(chosen(role))
    def _():
        edge_cells(nx, ny, cx, cy, *refs)


def edge_cells(
    nx, ny, cx, cy,
    own, got_a, got_b, plus, minus, back_plus, back_minus, back_y,
    hxa, hxb, hya, hyb, press, depth, sat, perm, pore, _,
    out,
):
    listing = blocks_of(own, got_a, got_b, plus, minus)
    sources = [(back_y, k * FLOW) for k in range(3)]
    sources += [(back_plus, k * FLOW) for k in range(3)]
    sources += [(back_minus, k * FLOW) for k in range(3)]
    home_x = lax.axis_index("gx")
    home_y = lax.axis_index("gy")
    columns = cx * cy

    def edge(first, second, dim, home, ends, rows_low, rows_high):
        even = lax.rem(home, 2) == 0
        for is_upper, rows in ((True, rows_high), (False, rows_low)):
            pick = even if is_upper else jnp.logical_not(even)
            far = [jnp.where(pick, first[f], second[f]) for f in range(5)]
            exists = (home < ends - 1) if is_upper else (home > 0)
            there = jnp.where(exists, 1.0, 0.0)
            mine, _, _ = load_state(press, depth, sat, rows)
            other = (far[0], far[1]) + mobility(far[2], far[3])
            trans = harmonic(perm[dim, rows, :], far[4]) * there
            if is_upper:
                flow = flux(mine, other, trans)
            else:
                flow = [-v for v in flux(other, mine, trans)]
            scale = STEP / pore[rows, :]
            for f in range(3):
                out[f, rows, :] = out[f, rows, :] - scale * flow[f]

    edge(hxa, hxb, 0, home_x, nx, pl.ds(0, cy), pl.ds(columns - cy, cy))
    edge(hya, hyb, 1, home_y, ny, pl.ds(0, cx, stride=cy), pl.ds(cy - 1, cx, stride=cy))
    for n, (ref, block) in enumerate(listing):
        meta = ref[META + block : META + block + 1, :].astype(jnp.int32)
        flows, row = sources[n]
        for rank in range(CAP):
            col = meta[0, rank]
            scale = STEP / pore[pl.ds(col, 1), :]
            for f in range(3):
                at = row + f * CAP + rank
                out[f, pl.ds(col, 1), :] = out[f, pl.ds(col, 1), :] + scale * flows[at : at + 1, :]


def finish_kernel(own, back_y, from_up, from_down, from_a, from_b, pore, _, out, work, sem):
    origin = own[META + 3 : META + 4, :].astype(jnp.int32)
    for ty in range(3):
        for tx in range(3):
            if ty > 0:
                ref, row = (from_a, from_b)[ty - 1], tx * FLOW
            elif tx == 0:
                ref, row = back_y, 0
            else:
                ref, row = (from_up, from_down)[tx - 1], 0
            for rank in range(CAP):
                col = origin[0, (ty * 3 + tx) * CAP + rank]
                scale = STEP / pore[pl.ds(col, 1), :]
                for f in range(3):
                    at = row + f * CAP + rank
                    work[f, pl.ds(col, 1), :] = (
                        work[f, pl.ds(col, 1), :] - scale * ref[at : at + 1, :]
                    )
    copy = pltpu.make_async_copy(work, out, sem)
    copy.start()
    copy.wait()


def swapped(value, axis, kind):
    count = lax.axis_size(axis)
    route = []
    for i in range(count):
        j = i ^ 1 if kind == 0 else (((i + 1) ^ 1) - 1) % count
        route.append((i, j))
    return lax.ppermute(value, axis, route)


def swapped_inside(value):
    nx, ny = lax.axis_size("gx"), lax.axis_size("gy")
    route = []
    for i in range(nx):
        for j in range(ny):
            if i in (0, nx - 1):
                route.append((i * ny + j, i * ny + (j ^ 1)))
            else:
                route.append((i * ny + j, (((i + 1) ^ 1) - 1) * ny + j))
    return lax.ppermute(value, ("gx", "gy"), route)


def shifted(value, axis, step):
    count = lax.axis_size(axis)
    return lax.ppermute(value, axis, [(i, (i + step) % count) for i in range(count)])


def relay_kernel(own, got_a, got_b, plus, minus):
    parts = (own, got_a, got_b)
    for tx, out in ((1, plus), (2, minus)):
        low = tx * BLOCK
        for k, part in enumerate(parts):
            out[k * BLOCK : (k + 1) * BLOCK, :] = part[low : low + BLOCK, :]
            out[META + k : META + k + 1, :] = part[META + tx : META + tx + 1, :]
        out[META + 3 :, :] = jnp.zeros((1, out.shape[1]), jnp.float32)


def relay_back_kernel(back_y, from_up, from_down, _, back_a, back_b):
    for ty, out in ((1, back_a), (2, back_b)):
        low = ty * FLOW
        for k, part in enumerate((back_y, from_up, from_down)):
            out[k * FLOW : (k + 1) * FLOW, :] = part[low : low + FLOW, :]
        out[3 * FLOW :, :] = jnp.zeros((BACK - 3 * FLOW, out.shape[1]), jnp.float32)


def step(
    pressure, depth, saturation, permeability, pore_volume,
    fault_pairs, fault_kind, fault_count, fault_table,
):
    cx, cy, layers = pressure.shape
    columns = cx * cy
    nx, ny = lax.axis_size("gx"), lax.axis_size("gy")
    f32 = jnp.float32
    slots = 9 * CAP
    rows = fault_pairs.shape[0]

    def flat(array):
        return array.reshape(array.shape[:-3] + (columns, layers))

    def cells(array):
        return array.reshape(array.shape[:-2] + (cx, cy, layers))

    def outer(array):
        return pltpu.with_memory_space_constraint(array, HBM)

    def vmem(*dims):
        return VMEM(dims, f32)

    message, back, full = vmem(ROWS, layers), vmem(BACK, layers), vmem(3, columns, layers)
    halo_x, halo_y = vmem(5, cy, layers), vmem(5, cx, layers)
    own, msg_a, msg_b, press, deep, sat = pl.pallas_call(
        functools.partial(pack_kernel, nx, ny),
        in_specs=[spec(HBM)] * 7,
        out_specs=[spec(VMEM)] * 6,
        out_shape=[message] * 3
        + [vmem(columns, layers)] * 2 + [vmem(2, columns, layers)],
        scratch_shapes=[
            SMEM((3, rows), jnp.int32), SMEM((rows,), jnp.int32), SMEM((1, 1), jnp.int32),
            SMEM((nx * ny,), jnp.int32),
            SMEM((slots,), jnp.int32), SMEM((slots,), jnp.int32), SMEM((slots,), jnp.int32),
            SMEM((slots,), jnp.int32), SMEM((slots,), jnp.int32),
            VMEM(fault_table.shape, f32),
            pltpu.SemaphoreType.DMA((4,)), pltpu.SemaphoreType.DMA((3,)),
        ],
        compiler_params=params(),
        cost_estimate=cost(4_000_000),
        name="pack",
    )(*map(lambda a: a if a.size <= 1 else outer(a), (
        fault_pairs.T, fault_kind, fault_count.reshape(1, 1), fault_table,
        flat(pressure), flat(depth), flat(saturation),
    )))
    perm, pore = flat(permeability), flat(pore_volume)

    cuts = (cx // 4, cx * 5 // 8)

    def stencil(first, last, role, base):
        operands = [press, deep, sat, perm, pore] + ([] if base is None else [base])
        return pl.pallas_call(
            functools.partial(stencil_kernel, cx, cy, first, last, role),
            in_specs=[spec(VMEM)] * 5 + ([] if base is None else [spec(pl.ANY)]),
            out_specs=spec(VMEM),
            out_shape=full,
            input_output_aliases={} if base is None else {5: 0},
            compiler_params=params(),
            cost_estimate=cost(8_000_000 * (last - first) // 8),
            name="stencil",
        )(*operands)

    def edges(role, base):
        return pl.pallas_call(
            functools.partial(edge_kernel, nx, ny, cx, cy, role),
            in_specs=[spec(VMEM)] * 18,
            out_specs=spec(VMEM),
            out_shape=full,
            input_output_aliases={17: 0},
            compiler_params=params(),
            cost_estimate=cost(4_000_000),
            name="edge",
        )(own, got_a, got_b, plus, minus, back_plus, back_minus, back_y,
          hxa, hxb, hya, hyb, press, deep, sat, perm, pore, base)

    got_b = swapped(msg_b, "gy", 1)
    got_a = swapped(msg_a, "gy", 0)
    base = stencil(0, cuts[0], None, None)
    hxa, hxb, hya, hyb = pl.pallas_call(
        functools.partial(halo_kernel, cx, cy),
        in_specs=[spec(VMEM)] * 4,
        out_specs=[spec(VMEM)] * 4,
        out_shape=[halo_x] * 2 + [halo_y] * 2,
        compiler_params=params(),
        cost_estimate=cost(100_000),
        name="halo",
    )(press, deep, sat, perm)
    plus, minus = pl.pallas_call(
        relay_kernel,
        in_specs=[spec(VMEM)] * 3,
        out_specs=[spec(VMEM)] * 2,
        out_shape=[message] * 2,
        compiler_params=params(),
        cost_estimate=cost(100_000),
        name="relay",
    )(own, got_a, got_b)
    plus = shifted(plus, "gx", 1)
    minus = shifted(minus, "gx", -1)
    base = stencil(cuts[0], cuts[1], None, base)
    back_plus, back_minus, back_y = pl.pallas_call(
        fault_kernel,
        in_specs=[spec(VMEM)] * 8 + [spec(pl.ANY)],
        out_specs=[spec(VMEM)] * 3,
        out_shape=[back] * 3,
        scratch_shapes=[VMEM((slots * 4, layers), f32)],
        compiler_params=params(),
        cost_estimate=cost(2_000_000),
        name="fault",
    )(own, got_a, got_b, plus, minus, press, deep, sat, base)
    from_down = shifted(back_minus, "gx", 1)
    base = stencil(cuts[1], cx, True, base)
    from_up = shifted(back_plus, "gx", -1)
    hxa = swapped(hxa, "gx", 0)
    hxb = swapped_inside(hxb)
    hyb = swapped(hyb, "gy", 1)
    hya = swapped(hya, "gy", 0)
    base = stencil(cuts[1], cx, False, base)
    back_a, back_b = pl.pallas_call(
        relay_back_kernel,
        in_specs=[spec(VMEM)] * 3 + [spec(pl.ANY)],
        out_specs=[spec(VMEM)] * 2,
        out_shape=[back] * 2,
        compiler_params=params(),
        cost_estimate=cost(100_000),
        name="relay_back",
    )(back_y, from_up, from_down, base)
    from_b = swapped(back_b, "gy", 1)
    from_a = swapped(back_a, "gy", 0)
    base = edges(None, base)
    out, _ = pl.pallas_call(
        finish_kernel,
        in_specs=[spec(VMEM)] * 8,
        out_specs=[spec(HBM), spec(VMEM)],
        out_shape=[jax.ShapeDtypeStruct((3, columns, layers), f32), full],
        input_output_aliases={7: 1},
        scratch_shapes=[pltpu.SemaphoreType.DMA],
        compiler_params=params(),
        cost_estimate=cost(2_000_000),
        name="finish",
    )(own, back_y, from_up, from_down, from_a, from_b, pore, base)
    return cells(out)


def solution(mesh):
    in_specs = (
        P("gx", "gy", None),
        P("gx", "gy", None),
        P(None, "gx", "gy", None),
        P(None, "gx", "gy", None),
        P("gx", "gy", None),
        P(("gx", "gy"), None),
        P(("gx", "gy")),
        P(("gx", "gy")),
        P(),
    )
    out_specs = P(None, "gx", "gy", None)
    return jax.shard_map(step, mesh=mesh, in_specs=in_specs, out_specs=out_specs, check_vma=False)
```

```python
import functools

import jax
import jax.numpy as jnp
from jax import lax
from jax.experimental import pallas as pl
from jax.experimental.pallas import tpu as pltpu
from jax.sharding import PartitionSpec as P


CAP = 4
FIELDS = 5
BLOCK = CAP * FIELDS
META = 3 * BLOCK
ROWS = 64
FLOW = 3 * CAP
BACK = 40

VISCOSITY = (0.5, 1.0, 0.25)
DENSITY = (1.0, 0.8, 0.25)
STEP = 0.2


VMEM = pltpu.VMEM
HBM = pltpu.HBM
SMEM = pltpu.SMEM


def spec(space):
    return pl.BlockSpec(memory_space=space)


def params(limit=6):
    return pltpu.CompilerParams(vmem_limit_bytes=limit * 2**20)


def cost(flops):
    return pl.CostEstimate(flops=flops, bytes_accessed=flops // 64, transcendentals=0)


def mobility(water, oil):
    gas = 1.0 - water - oil
    return (
        water * water * (1.0 / VISCOSITY[0]),
        oil * oil * (1.0 / VISCOSITY[1]),
        gas * gas * (1.0 / VISCOSITY[2]),
    )


def harmonic(first, second):
    return (first * second + first * second) / (first + second)


def flux(low, high, trans):
    dp = low[0] - high[0]
    dd = low[1] - high[1]
    flows = []
    for phase in range(3):
        drive = dp - DENSITY[phase] * dd if DENSITY[phase] != 1.0 else dp - dd
        up = jnp.where(drive > 0.0, low[2 + phase], high[2 + phase])
        flows.append(trans * drive * up)
    return flows


def pack_kernel(
    nx, ny,
    pairs_ref, kind_ref, count_ref, table_ref, press_f, depth_f, sat_f,
    own, msg_a, msg_b, press, depth, sat, src_s,
    pairs_s, kind_s, count_s, slot_s, seen_s, knd_s, liv_s, lnd_s, table,
    sem_i, sem_s,
):
    ints = [
        pltpu.make_async_copy(pairs_ref, pairs_s, sem_i.at[0]),
        pltpu.make_async_copy(kind_ref, kind_s, sem_i.at[1]),
        pltpu.make_async_copy(count_ref, count_s, sem_i.at[2]),
        pltpu.make_async_copy(table_ref, table, sem_i.at[3]),
    ]
    for copy in ints:
        copy.start()
    bulk = [
        pltpu.make_async_copy(press_f, press, sem_s.at[0]),
        pltpu.make_async_copy(depth_f, depth, sem_s.at[1]),
        pltpu.make_async_copy(sat_f, sat, sem_s.at[2]),
    ]
    for copy in bulk:
        copy.start()
    home_x = lax.axis_index("gx")
    home_y = lax.axis_index("gy")
    even_y = lax.rem(home_y, 2) == 0
    for step_x in (0, 1, -1):
        to_x = lax.rem(home_x + step_x + nx, nx)
        tx = step_x % 3
        for step_y in (0, 1, -1):
            to_y = lax.rem(home_y + step_y + ny, ny)
            if step_y == 0:
                ty = 0
            else:
                ty = jnp.where(even_y == (step_y == 1), 1, 2)
            slot_s[to_x * ny + to_y] = (ty * 3 + tx) * CAP
    for k in range(9 * CAP):
        seen_s[k] = 0
        src_s[k] = 0
        knd_s[k] = 0
        liv_s[k] = 0
        lnd_s[k] = 0
    for copy in ints:
        copy.wait()
    count = count_s[0, 0]
    for r in range(pairs_s.shape[1]):
        base = slot_s[pairs_s[1, r]]
        rank = seen_s[base]
        seen_s[base] = rank + 1
        position = base + rank
        src_s[position] = pairs_s[0, r]
        lnd_s[position] = pairs_s[2, r]
        knd_s[position] = kind_s[r]
        liv_s[position] = jnp.where(r < count, 1, 0)
    lane = lax.broadcasted_iota(jnp.int32, (1, own.shape[1]), 1)
    messages = (own, msg_a, msg_b)
    origin = jnp.zeros(lane.shape, jnp.int32)
    for ty in range(3):
        out = messages[ty]
        for tx in range(3):
            meta = jnp.zeros(lane.shape, jnp.int32)
            for rank in range(CAP):
                k = (ty * 3 + tx) * CAP + rank
                meta = jnp.where(lane == rank, lnd_s[k], meta)
                origin = jnp.where(lane == k, src_s[k], origin)
                trans = table[pl.ds(knd_s[k], 1), :]
                alive = liv_s[k].astype(jnp.float32)
                out[tx * BLOCK + 4 * CAP + rank : tx * BLOCK + 4 * CAP + rank + 1, :] = trans * alive
            out[META + tx : META + tx + 1, :] = meta.astype(jnp.float32)
        out[META + 3 : META + 4, :] = jnp.zeros(lane.shape, jnp.float32)
    own[META + 3 : META + 4, :] = origin.astype(jnp.float32)
    for copy in bulk:
        copy.wait()
    for ty in range(3):
        out = messages[ty]
        for tx in range(3):
            for rank in range(CAP):
                k = (ty * 3 + tx) * CAP + rank
                col = src_s[k]
                at = tx * BLOCK + rank
                out[at : at + 1, :] = press[pl.ds(col, 1), :]
                out[at + CAP : at + CAP + 1, :] = depth[pl.ds(col, 1), :]
                out[at + 2 * CAP : at + 2 * CAP + 1, :] = sat[0, pl.ds(col, 1), :]
                out[at + 3 * CAP : at + 3 * CAP + 1, :] = sat[1, pl.ds(col, 1), :]


def load_state(press, depth, sat, rows):
    water, oil = sat[0, rows, :], sat[1, rows, :]
    return (press[rows, :], depth[rows, :]) + mobility(water, oil), water, oil


def chosen(role):
    if role is None:
        return True
    return (lax.axis_index("gx") == 0) == role


def stencil_kernel(cx, cy, first, last, role, *refs):
    @pl.when(chosen(role))
    def _():
        stencil_rows(cx, cy, first, last, *refs)


def stencil_rows(cx, cy, first, last, *refs):
    press, depth, sat, perm, pore = refs[:5]
    out = refs[-1]
    lanes = press.shape[1]
    lane = lax.broadcasted_iota(jnp.int32, (8, lanes), 1)
    sub = lax.broadcasted_iota(jnp.int32, (8, lanes), 0)
    chunks = cy // 8

    def at(a, c, shift=0):
        return pl.ds(pl.multiple_of(a * cy, 8) + (c * 8 + shift), 8)

    def flow_x(a, c, low):
        rows = at(a + 1, c)
        high, _, _ = load_state(press, depth, sat, rows)
        trans = harmonic(perm[0, at(a, c), :], perm[0, rows, :])
        return flux(low, high, trans)

    def one_row(a, carry, top):
        out_carry = []
        below = None
        for c in range(chunks):
            rows = at(a, c)
            mine, water, oil = load_state(press, depth, sat, rows)
            if top:
                net = [-carry[3 * c + f] for f in range(3)]
            else:
                up = flow_x(a, c, mine)
                out_carry += up
                net = [up[f] - carry[3 * c + f] for f in range(3)]
            ky = perm[1, rows, :]
            if c < chunks - 1:
                rows_up = at(a, c, 1)
                high, _, _ = load_state(press, depth, sat, rows_up)
                trans = harmonic(ky, perm[1, rows_up, :])
            else:
                high = tuple(pltpu.roll(v, 7, 0) for v in mine)
                trans = jnp.where(sub < 7, harmonic(ky, pltpu.roll(ky, 7, 0)), 0.0)
            flow = flux(mine, high, trans)
            for f in range(3):
                back = pltpu.roll(flow[f], 1, 0)
                first_row = jnp.zeros_like(back) if c == 0 else below[f]
                net[f] = net[f] + (flow[f] - jnp.where(sub == 0, first_row, back))
            below = [pltpu.roll(flow[f], 1, 0) for f in range(3)]
            kz = perm[2, rows, :]
            high = tuple(pltpu.roll(v, lanes - 1, 1) for v in mine)
            trans = jnp.where(lane < lanes - 1, harmonic(kz, pltpu.roll(kz, lanes - 1, 1)), 0.0)
            flow = flux(mine, high, trans)
            for f in range(3):
                net[f] = net[f] + (flow[f] - pltpu.roll(flow[f], 1, 1))
            scale = STEP / pore[rows, :]
            gas = 1.0 - water - oil
            for f, now in enumerate((water, oil, gas)):
                out[f, rows, :] = now - scale * net[f]
        return tuple(out_carry)

    if first == 0:
        carry = tuple(jnp.zeros((8, lanes), jnp.float32) for _ in range(3 * chunks))
    else:
        carry = []
        for c in range(chunks):
            low, _, _ = load_state(press, depth, sat, at(first - 1, c))
            carry += flow_x(first - 1, c, low)
        carry = tuple(carry)
    end = min(last, cx - 1)
    carry = lax.fori_loop(first, end, lambda a, value: one_row(a, value, False), carry, unroll=2)
    if last == cx:
        one_row(cx - 1, carry, True)


def halo_kernel(cx, cy, press, depth, sat, perm, hxa, hxb, hya, hyb):
    even_x = lax.rem(lax.axis_index("gx"), 2) == 0
    even_y = lax.rem(lax.axis_index("gy"), 2) == 0
    columns = cx * cy
    low, high = pl.ds(0, cy), pl.ds(columns - cy, cy)
    left, right = pl.ds(0, cx, stride=cy), pl.ds(cy - 1, cx, stride=cy)
    for field in range(5):

        def rows(where, dim):
            if field < 2:
                return (press, depth)[field][where, :]
            return sat[field - 2, where, :] if field < 4 else perm[dim, where, :]

        first, last = rows(low, 0), rows(high, 0)
        hxa[field] = jnp.where(even_x, last, first)
        hxb[field] = jnp.where(even_x, first, last)
        first, last = rows(left, 1), rows(right, 1)
        hya[field] = jnp.where(even_y, last, first)
        hyb[field] = jnp.where(even_y, first, last)


def blocks_of(own, got_a, got_b, plus, minus):
    listing = [(own, 0), (got_a, 0), (got_b, 0)]
    listing += [(plus, b) for b in range(3)] + [(minus, b) for b in range(3)]
    return listing


def fault_kernel(
    own, got_a, got_b, plus, minus, press, depth, sat, _,
    back_plus, back_minus, back_y, local,
):
    listing = blocks_of(own, got_a, got_b, plus, minus)
    targets = [(back_y, k * FLOW) for k in range(3)]
    targets += [(back_plus, k * FLOW) for k in range(3)]
    targets += [(back_minus, k * FLOW) for k in range(3)]
    for n, (ref, block) in enumerate(listing):
        meta = ref[META + block : META + block + 1, :].astype(jnp.int32)
        for rank in range(CAP):
            col = meta[0, rank]
            at = n * 4 * CAP + rank
            local[at : at + 1, :] = press[pl.ds(col, 1), :]
            local[at + CAP : at + CAP + 1, :] = depth[pl.ds(col, 1), :]
            local[at + 2 * CAP : at + 2 * CAP + 1, :] = sat[0, pl.ds(col, 1), :]
            local[at + 3 * CAP : at + 3 * CAP + 1, :] = sat[1, pl.ds(col, 1), :]
    for n, (ref, block) in enumerate(listing):
        far = [ref[block * BLOCK + f * CAP : block * BLOCK + (f + 1) * CAP, :] for f in range(5)]
        near = [local[(n * 4 + f) * CAP : (n * 4 + f + 1) * CAP, :] for f in range(4)]
        flow = flux(
            (far[0], far[1]) + mobility(far[2], far[3]),
            (near[0], near[1]) + mobility(near[2], near[3]),
            far[4],
        )
        out, row = targets[n]
        for f in range(3):
            out[row + f * CAP : row + (f + 1) * CAP, :] = flow[f]
    for out in (back_plus, back_minus, back_y):
        out[3 * FLOW : BACK, :] = jnp.zeros((BACK - 3 * FLOW, out.shape[1]), jnp.float32)


def edge_kernel(nx, ny, cx, cy, role, *refs):
    @pl.when(chosen(role))
    def _():
        edge_cells(nx, ny, cx, cy, *refs)


def edge_cells(
    nx, ny, cx, cy,
    own, got_a, got_b, plus, minus, back_plus, back_minus, back_y,
    hxa, hxb, hya, hyb, press, depth, sat, perm, pore, _,
    out,
):
    listing = blocks_of(own, got_a, got_b, plus, minus)
    sources = [(back_y, k * FLOW) for k in range(3)]
    sources += [(back_plus, k * FLOW) for k in range(3)]
    sources += [(back_minus, k * FLOW) for k in range(3)]
    home_x = lax.axis_index("gx")
    home_y = lax.axis_index("gy")
    columns = cx * cy

    def edge(first, second, dim, home, ends, rows_low, rows_high):
        even = lax.rem(home, 2) == 0
        for is_upper, rows in ((True, rows_high), (False, rows_low)):
            pick = even if is_upper else jnp.logical_not(even)
            far = [jnp.where(pick, first[f], second[f]) for f in range(5)]
            exists = (home < ends - 1) if is_upper else (home > 0)
            there = jnp.where(exists, 1.0, 0.0)
            mine, _, _ = load_state(press, depth, sat, rows)
            other = (far[0], far[1]) + mobility(far[2], far[3])
            trans = harmonic(perm[dim, rows, :], far[4]) * there
            if is_upper:
                flow = flux(mine, other, trans)
            else:
                flow = [-v for v in flux(other, mine, trans)]
            scale = STEP / pore[rows, :]
            for f in range(3):
                out[f, rows, :] = out[f, rows, :] - scale * flow[f]

    edge(hxa, hxb, 0, home_x, nx, pl.ds(0, cy), pl.ds(columns - cy, cy))
    edge(hya, hyb, 1, home_y, ny, pl.ds(0, cx, stride=cy), pl.ds(cy - 1, cx, stride=cy))
    for n, (ref, block) in enumerate(listing):
        meta = ref[META + block : META + block + 1, :].astype(jnp.int32)
        flows, row = sources[n]
        for rank in range(CAP):
            col = meta[0, rank]
            scale = STEP / pore[pl.ds(col, 1), :]
            for f in range(3):
                at = row + f * CAP + rank
                out[f, pl.ds(col, 1), :] = out[f, pl.ds(col, 1), :] + scale * flows[at : at + 1, :]


def finish_kernel(origin, back_y, from_up, from_down, from_a, from_b, pore, _, out, work, sem):
    slots = []
    for ty in range(3):
        for tx in range(3):
            if ty > 0:
                ref, row = (from_a, from_b)[ty - 1], tx * FLOW
            elif tx == 0:
                ref, row = back_y, 0
            else:
                ref, row = (from_up, from_down)[tx - 1], 0
            for rank in range(CAP):
                col = origin[(ty * 3 + tx) * CAP + rank]
                slots.append((ref, row + rank, pl.ds(col, 1), STEP / pore[pl.ds(col, 1), :]))
    copies = []
    for f in range(3):
        for ref, row, col, scale in slots:
            at = row + f * CAP
            work[f, col, :] = work[f, col, :] - scale * ref[at : at + 1, :]
        copies.append(pltpu.make_async_copy(work.at[f], out.at[f], sem.at[f]))
        copies[-1].start()
    for copy in copies:
        copy.wait()


def swapped(value, axis, kind):
    count = lax.axis_size(axis)
    route = []
    for i in range(count):
        j = i ^ 1 if kind == 0 else (((i + 1) ^ 1) - 1) % count
        route.append((i, j))
    return lax.ppermute(value, axis, route)


def swapped_inside(value):
    nx, ny = lax.axis_size("gx"), lax.axis_size("gy")
    route = []
    for i in range(nx):
        for j in range(ny):
            if i in (0, nx - 1):
                route.append((i * ny + j, i * ny + (j ^ 1)))
            else:
                route.append((i * ny + j, (((i + 1) ^ 1) - 1) * ny + j))
    return lax.ppermute(value, ("gx", "gy"), route)


def shifted(value, axis, step):
    count = lax.axis_size(axis)
    return lax.ppermute(value, axis, [(i, (i + step) % count) for i in range(count)])


def relay_kernel(own, got_a, got_b, plus, minus):
    parts = (own, got_a, got_b)
    for tx, out in ((1, plus), (2, minus)):
        low = tx * BLOCK
        for k, part in enumerate(parts):
            out[k * BLOCK : (k + 1) * BLOCK, :] = part[low : low + BLOCK, :]
            out[META + k : META + k + 1, :] = part[META + tx : META + tx + 1, :]
        out[META + 3 :, :] = jnp.zeros((1, out.shape[1]), jnp.float32)


def relay_back_kernel(back_y, from_up, from_down, _, back_a, back_b):
    for ty, out in ((1, back_a), (2, back_b)):
        low = ty * FLOW
        for k, part in enumerate((back_y, from_up, from_down)):
            out[k * FLOW : (k + 1) * FLOW, :] = part[low : low + FLOW, :]
        out[3 * FLOW :, :] = jnp.zeros((BACK - 3 * FLOW, out.shape[1]), jnp.float32)


def step(
    pressure, depth, saturation, permeability, pore_volume,
    fault_pairs, fault_kind, fault_count, fault_table,
):
    cx, cy, layers = pressure.shape
    columns = cx * cy
    nx, ny = lax.axis_size("gx"), lax.axis_size("gy")
    f32 = jnp.float32
    slots = 9 * CAP
    rows = fault_pairs.shape[0]

    def flat(array):
        return array.reshape(array.shape[:-3] + (columns, layers))

    def cells(array):
        return array.reshape(array.shape[:-2] + (cx, cy, layers))

    def outer(array):
        return pltpu.with_memory_space_constraint(array, HBM)

    def vmem(*dims):
        return VMEM(dims, f32)

    message, back, full = vmem(ROWS, layers), vmem(BACK, layers), vmem(3, columns, layers)
    halo_x, halo_y = vmem(5, cy, layers), vmem(5, cx, layers)
    own, msg_a, msg_b, press, deep, sat, origin = pl.pallas_call(
        functools.partial(pack_kernel, nx, ny),
        in_specs=[spec(HBM)] * 7,
        out_specs=[spec(VMEM)] * 6 + [spec(SMEM)],
        out_shape=[message] * 3
        + [vmem(columns, layers)] * 2 + [vmem(2, columns, layers)] + [SMEM((slots,), jnp.int32)],
        scratch_shapes=[
            SMEM((3, rows), jnp.int32), SMEM((rows,), jnp.int32), SMEM((1, 1), jnp.int32),
            SMEM((nx * ny,), jnp.int32),
            SMEM((slots,), jnp.int32), SMEM((slots,), jnp.int32),
            SMEM((slots,), jnp.int32), SMEM((slots,), jnp.int32),
            VMEM(fault_table.shape, f32),
            pltpu.SemaphoreType.DMA((4,)), pltpu.SemaphoreType.DMA((3,)),
        ],
        compiler_params=params(),
        cost_estimate=cost(4_000_000),
        name="pack",
    )(*map(lambda a: a if a.size <= 1 else outer(a), (
        fault_pairs.T, fault_kind, fault_count.reshape(1, 1), fault_table,
        flat(pressure), flat(depth), flat(saturation),
    )))
    perm, pore = flat(permeability), flat(pore_volume)

    cuts = (cx // 4, cx * 5 // 8)

    def stencil(first, last, role, base):
        operands = [press, deep, sat, perm, pore] + ([] if base is None else [base])
        return pl.pallas_call(
            functools.partial(stencil_kernel, cx, cy, first, last, role),
            in_specs=[spec(VMEM)] * 5 + ([] if base is None else [spec(pl.ANY)]),
            out_specs=spec(VMEM),
            out_shape=full,
            input_output_aliases={} if base is None else {5: 0},
            compiler_params=params(),
            cost_estimate=cost(8_000_000 * (last - first) // 8),
            name="stencil",
        )(*operands)

    def edges(role, base):
        return pl.pallas_call(
            functools.partial(edge_kernel, nx, ny, cx, cy, role),
            in_specs=[spec(VMEM)] * 18,
            out_specs=spec(VMEM),
            out_shape=full,
            input_output_aliases={17: 0},
            compiler_params=params(),
            cost_estimate=cost(4_000_000),
            name="edge",
        )(own, got_a, got_b, plus, minus, back_plus, back_minus, back_y,
          hxa, hxb, hya, hyb, press, deep, sat, perm, pore, base)

    got_b = swapped(msg_b, "gy", 1)
    got_a = swapped(msg_a, "gy", 0)
    base = stencil(0, cuts[0], None, None)
    hxa, hxb, hya, hyb = pl.pallas_call(
        functools.partial(halo_kernel, cx, cy),
        in_specs=[spec(VMEM)] * 4,
        out_specs=[spec(VMEM)] * 4,
        out_shape=[halo_x] * 2 + [halo_y] * 2,
        compiler_params=params(),
        cost_estimate=cost(100_000),
        name="halo",
    )(press, deep, sat, perm)
    plus, minus = pl.pallas_call(
        relay_kernel,
        in_specs=[spec(VMEM)] * 3,
        out_specs=[spec(VMEM)] * 2,
        out_shape=[message] * 2,
        compiler_params=params(),
        cost_estimate=cost(100_000),
        name="relay",
    )(own, got_a, got_b)
    plus = shifted(plus, "gx", 1)
    minus = shifted(minus, "gx", -1)
    base = stencil(cuts[0], cuts[1], None, base)
    back_plus, back_minus, back_y = pl.pallas_call(
        fault_kernel,
        in_specs=[spec(VMEM)] * 8 + [spec(pl.ANY)],
        out_specs=[spec(VMEM)] * 3,
        out_shape=[back] * 3,
        scratch_shapes=[VMEM((slots * 4, layers), f32)],
        compiler_params=params(),
        cost_estimate=cost(2_000_000),
        name="fault",
    )(own, got_a, got_b, plus, minus, press, deep, sat, base)
    from_down = shifted(back_minus, "gx", 1)
    base = stencil(cuts[1], cx, True, base)
    from_up = shifted(back_plus, "gx", -1)
    hxa = swapped(hxa, "gx", 0)
    hxb = swapped_inside(hxb)
    hyb = swapped(hyb, "gy", 1)
    hya = swapped(hya, "gy", 0)
    base = stencil(cuts[1], cx, False, base)
    back_a, back_b = pl.pallas_call(
        relay_back_kernel,
        in_specs=[spec(VMEM)] * 3 + [spec(pl.ANY)],
        out_specs=[spec(VMEM)] * 2,
        out_shape=[back] * 2,
        compiler_params=params(),
        cost_estimate=cost(100_000),
        name="relay_back",
    )(back_y, from_up, from_down, base)
    from_b = swapped(back_b, "gy", 1)
    from_a = swapped(back_a, "gy", 0)
    base = edges(None, base)
    out, _ = pl.pallas_call(
        finish_kernel,
        in_specs=[spec(SMEM)] + [spec(VMEM)] * 7,
        out_specs=[spec(HBM), spec(VMEM)],
        out_shape=[jax.ShapeDtypeStruct((3, columns, layers), f32), full],
        input_output_aliases={7: 1},
        scratch_shapes=[pltpu.SemaphoreType.DMA((3,))],
        compiler_params=params(),
        cost_estimate=cost(2_000_000),
        name="finish",
    )(origin, back_y, from_up, from_down, from_a, from_b, pore, base)
    return cells(out)


def solution(mesh):
    in_specs = (
        P("gx", "gy", None),
        P("gx", "gy", None),
        P(None, "gx", "gy", None),
        P(None, "gx", "gy", None),
        P("gx", "gy", None),
        P(("gx", "gy"), None),
        P(("gx", "gy")),
        P(("gx", "gy")),
        P(),
    )
    out_specs = P(None, "gx", "gy", None)
    return jax.shard_map(step, mesh=mesh, in_specs=in_specs, out_specs=out_specs, check_vma=False)
```

```python
import functools

import jax
import jax.numpy as jnp
from jax import lax
from jax.experimental import pallas as pl
from jax.experimental.pallas import tpu as pltpu
from jax.sharding import PartitionSpec as P


CAP = 4
FIELDS = 5
BLOCK = CAP * FIELDS
META = 3 * BLOCK
ROWS = 64
FLOW = 3 * CAP
BACK = 40

VISCOSITY = (0.5, 1.0, 0.25)
DENSITY = (1.0, 0.8, 0.25)
STEP = 0.2


VMEM = pltpu.VMEM
HBM = pltpu.HBM
SMEM = pltpu.SMEM


def spec(space):
    return pl.BlockSpec(memory_space=space)


def params(limit=6):
    return pltpu.CompilerParams(vmem_limit_bytes=limit * 2**20)


def cost(flops):
    return pl.CostEstimate(flops=flops, bytes_accessed=flops // 64, transcendentals=0)


def mobility(water, oil):
    gas = 1.0 - water - oil
    return (
        water * water * (1.0 / VISCOSITY[0]),
        oil * oil * (1.0 / VISCOSITY[1]),
        gas * gas * (1.0 / VISCOSITY[2]),
    )


def harmonic(first, second):
    return (first * second + first * second) / (first + second)


def flux(low, high, trans):
    dp = low[0] - high[0]
    dd = low[1] - high[1]
    flows = []
    for phase in range(3):
        drive = dp - DENSITY[phase] * dd if DENSITY[phase] != 1.0 else dp - dd
        up = jnp.where(drive > 0.0, low[2 + phase], high[2 + phase])
        flows.append(trans * drive * up)
    return flows


def pack_kernel(
    nx, ny,
    pairs_ref, kind_ref, count_ref, table_ref, press_f, depth_f, sat_f,
    own, msg_a, msg_b, press, depth, sat, src_s,
    pairs_s, kind_s, count_s, slot_s, knd_s, lnd_s, table,
    sem_i, sem_s,
):
    ints = [
        pltpu.make_async_copy(pairs_ref, pairs_s, sem_i.at[0]),
        pltpu.make_async_copy(kind_ref, kind_s, sem_i.at[1]),
        pltpu.make_async_copy(count_ref, count_s, sem_i.at[2]),
        pltpu.make_async_copy(table_ref, table.at[pl.ds(0, table_ref.shape[0])], sem_i.at[3]),
    ]
    for copy in ints:
        copy.start()
    bulk = [
        pltpu.make_async_copy(press_f, press, sem_s.at[0]),
        pltpu.make_async_copy(depth_f, depth, sem_s.at[1]),
        pltpu.make_async_copy(sat_f, sat, sem_s.at[2]),
    ]
    for copy in bulk:
        copy.start()
    home_x = lax.axis_index("gx")
    home_y = lax.axis_index("gy")
    even_y = lax.rem(home_y, 2) == 0
    for step_x in (0, 1, -1):
        to_x = lax.rem(home_x + step_x + nx, nx)
        tx = step_x % 3
        for step_y in (0, 1, -1):
            to_y = lax.rem(home_y + step_y + ny, ny)
            if step_y == 0:
                ty = 0
            else:
                ty = jnp.where(even_y == (step_y == 1), 1, 2)
            slot_s[to_x * ny + to_y] = ty * 3 + tx
    kinds = table_ref.shape[0]
    table[kinds:, :] = jnp.zeros((table.shape[0] - kinds, table.shape[1]), jnp.float32)
    for k in range(9 * CAP):
        src_s[k] = 0
        knd_s[k] = kinds
        lnd_s[k] = 0
    for copy in ints:
        copy.wait()
    count = count_s[0, 0]
    seen = jnp.int32(0)
    for r in range(pairs_s.shape[1]):
        block = slot_s[pairs_s[1, r]]
        shift = 3 * block
        rank = lax.shift_right_logical(seen, shift) & 7
        seen = seen + lax.shift_left(jnp.int32(1), shift)
        position = block * CAP + rank
        src_s[position] = pairs_s[0, r]
        lnd_s[position] = pairs_s[2, r]
        knd_s[position] = jnp.where(r < count, kind_s[r], kinds)
    lane = lax.broadcasted_iota(jnp.int32, (1, own.shape[1]), 1)
    messages = (own, msg_a, msg_b)
    origin = jnp.zeros(lane.shape, jnp.int32)
    for ty in range(3):
        out = messages[ty]
        for tx in range(3):
            meta = jnp.zeros(lane.shape, jnp.int32)
            for rank in range(CAP):
                k = (ty * 3 + tx) * CAP + rank
                meta = jnp.where(lane == rank, lnd_s[k], meta)
                origin = jnp.where(lane == k, src_s[k], origin)
                trans = table[pl.ds(knd_s[k], 1), :]
                out[tx * BLOCK + 4 * CAP + rank : tx * BLOCK + 4 * CAP + rank + 1, :] = trans
            out[META + tx : META + tx + 1, :] = meta.astype(jnp.float32)
        out[META + 3 : META + 4, :] = jnp.zeros(lane.shape, jnp.float32)
    own[META + 3 : META + 4, :] = origin.astype(jnp.float32)
    for copy in bulk:
        copy.wait()
    for ty in range(3):
        out = messages[ty]
        for tx in range(3):
            for rank in range(CAP):
                k = (ty * 3 + tx) * CAP + rank
                col = src_s[k]
                at = tx * BLOCK + rank
                out[at : at + 1, :] = press[pl.ds(col, 1), :]
                out[at + CAP : at + CAP + 1, :] = depth[pl.ds(col, 1), :]
                out[at + 2 * CAP : at + 2 * CAP + 1, :] = sat[0, pl.ds(col, 1), :]
                out[at + 3 * CAP : at + 3 * CAP + 1, :] = sat[1, pl.ds(col, 1), :]


def load_state(press, depth, sat, rows):
    water, oil = sat[0, rows, :], sat[1, rows, :]
    return (press[rows, :], depth[rows, :]) + mobility(water, oil), water, oil


def chosen(role):
    if role is None:
        return True
    return (lax.axis_index("gx") == 0) == role


def stencil_kernel(cx, cy, first, last, role, *refs):
    @pl.when(chosen(role))
    def _():
        stencil_rows(cx, cy, first, last, *refs)


def stencil_rows(cx, cy, first, last, *refs):
    press, depth, sat, perm, pore = refs[:5]
    out = refs[-1]
    lanes = press.shape[1]
    lane = lax.broadcasted_iota(jnp.int32, (8, lanes), 1)
    sub = lax.broadcasted_iota(jnp.int32, (8, lanes), 0)
    chunks = cy // 8

    def at(a, c, shift=0):
        return pl.ds(pl.multiple_of(a * cy, 8) + (c * 8 + shift), 8)

    def flow_x(a, c, low):
        rows = at(a + 1, c)
        high, _, _ = load_state(press, depth, sat, rows)
        trans = harmonic(perm[0, at(a, c), :], perm[0, rows, :])
        return flux(low, high, trans)

    def one_row(a, carry, top):
        out_carry = []
        below = None
        for c in range(chunks):
            rows = at(a, c)
            mine, water, oil = load_state(press, depth, sat, rows)
            if top:
                net = [-carry[3 * c + f] for f in range(3)]
            else:
                up = flow_x(a, c, mine)
                out_carry += up
                net = [up[f] - carry[3 * c + f] for f in range(3)]
            ky = perm[1, rows, :]
            if c < chunks - 1:
                rows_up = at(a, c, 1)
                high, _, _ = load_state(press, depth, sat, rows_up)
                trans = harmonic(ky, perm[1, rows_up, :])
            else:
                high = tuple(pltpu.roll(v, 7, 0) for v in mine)
                trans = jnp.where(sub < 7, harmonic(ky, pltpu.roll(ky, 7, 0)), 0.0)
            flow = flux(mine, high, trans)
            for f in range(3):
                back = pltpu.roll(flow[f], 1, 0)
                first_row = jnp.zeros_like(back) if c == 0 else below[f]
                net[f] = net[f] + (flow[f] - jnp.where(sub == 0, first_row, back))
            below = [pltpu.roll(flow[f], 1, 0) for f in range(3)]
            kz = perm[2, rows, :]
            high = tuple(pltpu.roll(v, lanes - 1, 1) for v in mine)
            trans = jnp.where(lane < lanes - 1, harmonic(kz, pltpu.roll(kz, lanes - 1, 1)), 0.0)
            flow = flux(mine, high, trans)
            for f in range(3):
                net[f] = net[f] + (flow[f] - pltpu.roll(flow[f], 1, 1))
            scale = STEP / pore[rows, :]
            gas = 1.0 - water - oil
            for f, now in enumerate((water, oil, gas)):
                out[f, rows, :] = now - scale * net[f]
        return tuple(out_carry)

    if first == 0:
        carry = tuple(jnp.zeros((8, lanes), jnp.float32) for _ in range(3 * chunks))
    else:
        carry = []
        for c in range(chunks):
            low, _, _ = load_state(press, depth, sat, at(first - 1, c))
            carry += flow_x(first - 1, c, low)
        carry = tuple(carry)
    end = min(last, cx - 1)
    carry = lax.fori_loop(first, end, lambda a, value: one_row(a, value, False), carry, unroll=2)
    if last == cx:
        one_row(cx - 1, carry, True)


def halo_kernel(cx, cy, press, depth, sat, perm, hxa, hxb, hya, hyb):
    even_x = lax.rem(lax.axis_index("gx"), 2) == 0
    even_y = lax.rem(lax.axis_index("gy"), 2) == 0
    columns = cx * cy
    low, high = pl.ds(0, cy), pl.ds(columns - cy, cy)
    left, right = pl.ds(0, cx, stride=cy), pl.ds(cy - 1, cx, stride=cy)
    for field in range(5):

        def rows(where, dim):
            if field < 2:
                return (press, depth)[field][where, :]
            return sat[field - 2, where, :] if field < 4 else perm[dim, where, :]

        first, last = rows(low, 0), rows(high, 0)
        hxa[field] = jnp.where(even_x, last, first)
        hxb[field] = jnp.where(even_x, first, last)
        first, last = rows(left, 1), rows(right, 1)
        hya[field] = jnp.where(even_y, last, first)
        hyb[field] = jnp.where(even_y, first, last)


def blocks_of(own, got_a, got_b, plus, minus):
    listing = [(own, 0), (got_a, 0), (got_b, 0)]
    listing += [(plus, b) for b in range(3)] + [(minus, b) for b in range(3)]
    return listing


def fault_kernel(
    own, got_a, got_b, plus, minus, press, depth, sat, _,
    back_plus, back_minus, back_y, local,
):
    listing = blocks_of(own, got_a, got_b, plus, minus)
    targets = [(back_y, k * FLOW) for k in range(3)]
    targets += [(back_plus, k * FLOW) for k in range(3)]
    targets += [(back_minus, k * FLOW) for k in range(3)]
    for n, (ref, block) in enumerate(listing):
        meta = ref[META + block : META + block + 1, :].astype(jnp.int32)
        for rank in range(CAP):
            col = meta[0, rank]
            at = n * 4 * CAP + rank
            local[at : at + 1, :] = press[pl.ds(col, 1), :]
            local[at + CAP : at + CAP + 1, :] = depth[pl.ds(col, 1), :]
            local[at + 2 * CAP : at + 2 * CAP + 1, :] = sat[0, pl.ds(col, 1), :]
            local[at + 3 * CAP : at + 3 * CAP + 1, :] = sat[1, pl.ds(col, 1), :]
    for n, (ref, block) in enumerate(listing):
        far = [ref[block * BLOCK + f * CAP : block * BLOCK + (f + 1) * CAP, :] for f in range(5)]
        near = [local[(n * 4 + f) * CAP : (n * 4 + f + 1) * CAP, :] for f in range(4)]
        flow = flux(
            (far[0], far[1]) + mobility(far[2], far[3]),
            (near[0], near[1]) + mobility(near[2], near[3]),
            far[4],
        )
        out, row = targets[n]
        for f in range(3):
            out[row + f * CAP : row + (f + 1) * CAP, :] = flow[f]
    for out in (back_plus, back_minus, back_y):
        out[3 * FLOW : BACK, :] = jnp.zeros((BACK - 3 * FLOW, out.shape[1]), jnp.float32)


def edge_kernel(nx, ny, cx, cy, role, *refs):
    @pl.when(chosen(role))
    def _():
        edge_cells(nx, ny, cx, cy, *refs)


def edge_cells(
    nx, ny, cx, cy,
    own, got_a, got_b, plus, minus, back_plus, back_minus, back_y,
    hxa, hxb, hya, hyb, press, depth, sat, perm, pore, _,
    out,
):
    listing = blocks_of(own, got_a, got_b, plus, minus)
    sources = [(back_y, k * FLOW) for k in range(3)]
    sources += [(back_plus, k * FLOW) for k in range(3)]
    sources += [(back_minus, k * FLOW) for k in range(3)]
    home_x = lax.axis_index("gx")
    home_y = lax.axis_index("gy")
    columns = cx * cy

    def edge(first, second, dim, home, ends, rows_low, rows_high):
        even = lax.rem(home, 2) == 0
        for is_upper, rows in ((True, rows_high), (False, rows_low)):
            pick = even if is_upper else jnp.logical_not(even)
            far = [jnp.where(pick, first[f], second[f]) for f in range(5)]
            exists = (home < ends - 1) if is_upper else (home > 0)
            there = jnp.where(exists, 1.0, 0.0)
            mine, _, _ = load_state(press, depth, sat, rows)
            other = (far[0], far[1]) + mobility(far[2], far[3])
            trans = harmonic(perm[dim, rows, :], far[4]) * there
            if is_upper:
                flow = flux(mine, other, trans)
            else:
                flow = [-v for v in flux(other, mine, trans)]
            scale = STEP / pore[rows, :]
            for f in range(3):
                out[f, rows, :] = out[f, rows, :] - scale * flow[f]

    edge(hxa, hxb, 0, home_x, nx, pl.ds(0, cy), pl.ds(columns - cy, cy))
    edge(hya, hyb, 1, home_y, ny, pl.ds(0, cx, stride=cy), pl.ds(cy - 1, cx, stride=cy))
    for n, (ref, block) in enumerate(listing):
        meta = ref[META + block : META + block + 1, :].astype(jnp.int32)
        flows, row = sources[n]
        for rank in range(CAP):
            col = meta[0, rank]
            scale = STEP / pore[pl.ds(col, 1), :]
            for f in range(3):
                at = row + f * CAP + rank
                out[f, pl.ds(col, 1), :] = out[f, pl.ds(col, 1), :] + scale * flows[at : at + 1, :]


def finish_kernel(origin, back_y, from_up, from_down, from_a, from_b, pore, _, out, work, sem):
    slots = []
    for ty in range(3):
        for tx in range(3):
            if ty > 0:
                ref, row = (from_a, from_b)[ty - 1], tx * FLOW
            elif tx == 0:
                ref, row = back_y, 0
            else:
                ref, row = (from_up, from_down)[tx - 1], 0
            for rank in range(CAP):
                col = origin[(ty * 3 + tx) * CAP + rank]
                slots.append((ref, row + rank, pl.ds(col, 1), STEP / pore[pl.ds(col, 1), :]))
    copies = []
    for f in range(3):
        for ref, row, col, scale in slots:
            at = row + f * CAP
            work[f, col, :] = work[f, col, :] - scale * ref[at : at + 1, :]
        copies.append(pltpu.make_async_copy(work.at[f], out.at[f], sem.at[f]))
        copies[-1].start()
    for copy in copies:
        copy.wait()


def swapped(value, axis, kind):
    count = lax.axis_size(axis)
    route = []
    for i in range(count):
        j = i ^ 1 if kind == 0 else (((i + 1) ^ 1) - 1) % count
        route.append((i, j))
    return lax.ppermute(value, axis, route)


def swapped_inside(value):
    nx, ny = lax.axis_size("gx"), lax.axis_size("gy")
    route = []
    for i in range(nx):
        for j in range(ny):
            if i in (0, nx - 1):
                route.append((i * ny + j, i * ny + (j ^ 1)))
            else:
                route.append((i * ny + j, (((i + 1) ^ 1) - 1) * ny + j))
    return lax.ppermute(value, ("gx", "gy"), route)


def shifted(value, axis, step):
    count = lax.axis_size(axis)
    return lax.ppermute(value, axis, [(i, (i + step) % count) for i in range(count)])


def relay_kernel(own, got_a, got_b, plus, minus):
    parts = (own, got_a, got_b)
    for tx, out in ((1, plus), (2, minus)):
        low = tx * BLOCK
        for k, part in enumerate(parts):
            out[k * BLOCK : (k + 1) * BLOCK, :] = part[low : low + BLOCK, :]
            out[META + k : META + k + 1, :] = part[META + tx : META + tx + 1, :]
        out[META + 3 :, :] = jnp.zeros((1, out.shape[1]), jnp.float32)


def relay_back_kernel(back_y, from_up, from_down, _, back_a, back_b):
    for ty, out in ((1, back_a), (2, back_b)):
        low = ty * FLOW
        for k, part in enumerate((back_y, from_up, from_down)):
            out[k * FLOW : (k + 1) * FLOW, :] = part[low : low + FLOW, :]
        out[3 * FLOW :, :] = jnp.zeros((BACK - 3 * FLOW, out.shape[1]), jnp.float32)


def step(
    pressure, depth, saturation, permeability, pore_volume,
    fault_pairs, fault_kind, fault_count, fault_table,
):
    cx, cy, layers = pressure.shape
    columns = cx * cy
    nx, ny = lax.axis_size("gx"), lax.axis_size("gy")
    f32 = jnp.float32
    slots = 9 * CAP
    rows = fault_pairs.shape[0]

    def flat(array):
        return array.reshape(array.shape[:-3] + (columns, layers))

    def cells(array):
        return array.reshape(array.shape[:-2] + (cx, cy, layers))

    def outer(array):
        return pltpu.with_memory_space_constraint(array, HBM)

    def vmem(*dims):
        return VMEM(dims, f32)

    message, back, full = vmem(ROWS, layers), vmem(BACK, layers), vmem(3, columns, layers)
    halo_x, halo_y = vmem(5, cy, layers), vmem(5, cx, layers)
    own, msg_a, msg_b, press, deep, sat, origin = pl.pallas_call(
        functools.partial(pack_kernel, nx, ny),
        in_specs=[spec(HBM)] * 7,
        out_specs=[spec(VMEM)] * 6 + [spec(SMEM)],
        out_shape=[message] * 3
        + [vmem(columns, layers)] * 2 + [vmem(2, columns, layers)] + [SMEM((slots,), jnp.int32)],
        scratch_shapes=[
            SMEM((3, rows), jnp.int32), SMEM((rows,), jnp.int32), SMEM((1, 1), jnp.int32),
            SMEM((nx * ny,), jnp.int32),
            SMEM((slots,), jnp.int32), SMEM((slots,), jnp.int32),
            VMEM((fault_table.shape[0] + 8, layers), f32),
            pltpu.SemaphoreType.DMA((4,)), pltpu.SemaphoreType.DMA((3,)),
        ],
        compiler_params=params(),
        cost_estimate=cost(4_000_000),
        name="pack",
    )(*map(lambda a: a if a.size <= 1 else outer(a), (
        fault_pairs.T, fault_kind, fault_count.reshape(1, 1), fault_table,
        flat(pressure), flat(depth), flat(saturation),
    )))
    perm, pore = flat(permeability), flat(pore_volume)

    cuts = (cx // 4, cx * 5 // 8)

    def stencil(first, last, role, base):
        operands = [press, deep, sat, perm, pore] + ([] if base is None else [base])
        return pl.pallas_call(
            functools.partial(stencil_kernel, cx, cy, first, last, role),
            in_specs=[spec(VMEM)] * 5 + ([] if base is None else [spec(pl.ANY)]),
            out_specs=spec(VMEM),
            out_shape=full,
            input_output_aliases={} if base is None else {5: 0},
            compiler_params=params(),
            cost_estimate=cost(8_000_000 * (last - first) // 8),
            name="stencil",
        )(*operands)

    def edges(role, base):
        return pl.pallas_call(
            functools.partial(edge_kernel, nx, ny, cx, cy, role),
            in_specs=[spec(VMEM)] * 18,
            out_specs=spec(VMEM),
            out_shape=full,
            input_output_aliases={17: 0},
            compiler_params=params(),
            cost_estimate=cost(4_000_000),
            name="edge",
        )(own, got_a, got_b, plus, minus, back_plus, back_minus, back_y,
          hxa, hxb, hya, hyb, press, deep, sat, perm, pore, base)

    got_b = swapped(msg_b, "gy", 1)
    got_a = swapped(msg_a, "gy", 0)
    base = stencil(0, cuts[0], None, None)
    hxa, hxb, hya, hyb = pl.pallas_call(
        functools.partial(halo_kernel, cx, cy),
        in_specs=[spec(VMEM)] * 4,
        out_specs=[spec(VMEM)] * 4,
        out_shape=[halo_x] * 2 + [halo_y] * 2,
        compiler_params=params(),
        cost_estimate=cost(100_000),
        name="halo",
    )(press, deep, sat, perm)
    plus, minus = pl.pallas_call(
        relay_kernel,
        in_specs=[spec(VMEM)] * 3,
        out_specs=[spec(VMEM)] * 2,
        out_shape=[message] * 2,
        compiler_params=params(),
        cost_estimate=cost(100_000),
        name="relay",
    )(own, got_a, got_b)
    plus = shifted(plus, "gx", 1)
    minus = shifted(minus, "gx", -1)
    base = stencil(cuts[0], cuts[1], None, base)
    back_plus, back_minus, back_y = pl.pallas_call(
        fault_kernel,
        in_specs=[spec(VMEM)] * 8 + [spec(pl.ANY)],
        out_specs=[spec(VMEM)] * 3,
        out_shape=[back] * 3,
        scratch_shapes=[VMEM((slots * 4, layers), f32)],
        compiler_params=params(),
        cost_estimate=cost(2_000_000),
        name="fault",
    )(own, got_a, got_b, plus, minus, press, deep, sat, base)
    from_down = shifted(back_minus, "gx", 1)
    base = stencil(cuts[1], cx, True, base)
    from_up = shifted(back_plus, "gx", -1)
    hxa = swapped(hxa, "gx", 0)
    hxb = swapped_inside(hxb)
    hyb = swapped(hyb, "gy", 1)
    hya = swapped(hya, "gy", 0)
    base = stencil(cuts[1], cx, False, base)
    back_a, back_b = pl.pallas_call(
        relay_back_kernel,
        in_specs=[spec(VMEM)] * 3 + [spec(pl.ANY)],
        out_specs=[spec(VMEM)] * 2,
        out_shape=[back] * 2,
        compiler_params=params(),
        cost_estimate=cost(100_000),
        name="relay_back",
    )(back_y, from_up, from_down, base)
    from_b = swapped(back_b, "gy", 1)
    from_a = swapped(back_a, "gy", 0)
    base = edges(None, base)
    out, _ = pl.pallas_call(
        finish_kernel,
        in_specs=[spec(SMEM)] + [spec(VMEM)] * 7,
        out_specs=[spec(HBM), spec(VMEM)],
        out_shape=[jax.ShapeDtypeStruct((3, columns, layers), f32), full],
        input_output_aliases={7: 1},
        scratch_shapes=[pltpu.SemaphoreType.DMA((3,))],
        compiler_params=params(),
        cost_estimate=cost(2_000_000),
        name="finish",
    )(origin, back_y, from_up, from_down, from_a, from_b, pore, base)
    return cells(out)


def solution(mesh):
    in_specs = (
        P("gx", "gy", None),
        P("gx", "gy", None),
        P(None, "gx", "gy", None),
        P(None, "gx", "gy", None),
        P("gx", "gy", None),
        P(("gx", "gy"), None),
        P(("gx", "gy")),
        P(("gx", "gy")),
        P(),
    )
    out_specs = P(None, "gx", "gy", None)
    return jax.shard_map(step, mesh=mesh, in_specs=in_specs, out_specs=out_specs, check_vma=False)
```

```python
import functools

import jax
import jax.numpy as jnp
from jax import lax
from jax.experimental import pallas as pl
from jax.experimental.pallas import tpu as pltpu
from jax.sharding import PartitionSpec as P


CAP = 4
FIELDS = 5
BLOCK = CAP * FIELDS
META = 3 * BLOCK
ROWS = 64
FLOW = 3 * CAP
BACK = 40

VISCOSITY = (0.5, 1.0, 0.25)
DENSITY = (1.0, 0.8, 0.25)
STEP = 0.2


VMEM = pltpu.VMEM
HBM = pltpu.HBM
SMEM = pltpu.SMEM


def spec(space):
    return pl.BlockSpec(memory_space=space)


def params(limit=6):
    return pltpu.CompilerParams(vmem_limit_bytes=limit * 2**20)


def cost(flops):
    return pl.CostEstimate(flops=flops, bytes_accessed=flops // 64, transcendentals=0)


def mobility(water, oil):
    gas = 1.0 - water - oil
    return (
        water * water * (1.0 / VISCOSITY[0]),
        oil * oil * (1.0 / VISCOSITY[1]),
        gas * gas * (1.0 / VISCOSITY[2]),
    )


def harmonic(first, second):
    return (first * second + first * second) / (first + second)


def flux(low, high, trans):
    dp = low[0] - high[0]
    dd = low[1] - high[1]
    flows = []
    for phase in range(3):
        drive = dp - DENSITY[phase] * dd if DENSITY[phase] != 1.0 else dp - dd
        up = jnp.where(drive > 0.0, low[2 + phase], high[2 + phase])
        flows.append(trans * drive * up)
    return flows


def pack_kernel(
    nx, ny,
    pairs_ref, kind_ref, count_ref, table_ref, press_f, depth_f, sat_f,
    own, msg_a, msg_b, press, depth, sat, src_s,
    pairs_s, kind_s, count_s, slot_s, knd_s, lnd_s, table,
    sem_i, sem_s,
):
    ints = [
        pltpu.make_async_copy(pairs_ref, pairs_s, sem_i.at[0]),
        pltpu.make_async_copy(kind_ref, kind_s, sem_i.at[1]),
        pltpu.make_async_copy(count_ref, count_s, sem_i.at[2]),
        pltpu.make_async_copy(table_ref, table.at[pl.ds(0, table_ref.shape[0])], sem_i.at[3]),
    ]
    for copy in ints:
        copy.start()
    bulk = [
        pltpu.make_async_copy(press_f, press, sem_s.at[0]),
        pltpu.make_async_copy(depth_f, depth, sem_s.at[1]),
        pltpu.make_async_copy(sat_f, sat, sem_s.at[2]),
    ]
    for copy in bulk:
        copy.start()
    home_x = lax.axis_index("gx")
    home_y = lax.axis_index("gy")
    even_y = lax.rem(home_y, 2) == 0
    for step_x in (0, 1, -1):
        to_x = lax.rem(home_x + step_x + nx, nx)
        tx = step_x % 3
        for step_y in (0, 1, -1):
            to_y = lax.rem(home_y + step_y + ny, ny)
            if step_y == 0:
                ty = 0
            else:
                ty = jnp.where(even_y == (step_y == 1), 1, 2)
            slot_s[to_x * ny + to_y] = ty * 3 + tx
    kinds = table_ref.shape[0]
    table[kinds:, :] = jnp.zeros((table.shape[0] - kinds, table.shape[1]), jnp.float32)
    for k in range(9 * CAP):
        src_s[k] = 0
        knd_s[k] = kinds
        lnd_s[k] = 0
    for copy in ints:
        copy.wait()
    count = count_s[0, 0]
    seen = jnp.int32(0)
    for r in range(pairs_s.shape[1]):
        block = slot_s[pairs_s[1, r]]
        shift = 3 * block
        rank = lax.shift_right_logical(seen, shift) & 7
        seen = seen + lax.shift_left(jnp.int32(1), shift)
        position = block * CAP + rank
        src_s[position] = pairs_s[0, r]
        lnd_s[position] = pairs_s[2, r]
        knd_s[position] = jnp.where(r < count, kind_s[r], kinds)
    lane = lax.broadcasted_iota(jnp.int32, (1, own.shape[1]), 1)
    messages = (own, msg_a, msg_b)
    for ty in range(3):
        out = messages[ty]
        for tx in range(3):
            meta = jnp.zeros(lane.shape, jnp.int32)
            for rank in range(CAP):
                k = (ty * 3 + tx) * CAP + rank
                meta = jnp.where(lane == rank, lnd_s[k], meta)
                trans = table[pl.ds(knd_s[k], 1), :]
                out[tx * BLOCK + 4 * CAP + rank : tx * BLOCK + 4 * CAP + rank + 1, :] = trans
            out[META + tx : META + tx + 1, :] = meta.astype(jnp.float32)
        out[META + 3 : META + 4, :] = jnp.zeros(lane.shape, jnp.float32)
    for copy in bulk:
        copy.wait()
    for ty in range(3):
        out = messages[ty]
        for tx in range(3):
            for rank in range(CAP):
                k = (ty * 3 + tx) * CAP + rank
                col = src_s[k]
                at = tx * BLOCK + rank
                out[at : at + 1, :] = press[pl.ds(col, 1), :]
                out[at + CAP : at + CAP + 1, :] = depth[pl.ds(col, 1), :]
                out[at + 2 * CAP : at + 2 * CAP + 1, :] = sat[0, pl.ds(col, 1), :]
                out[at + 3 * CAP : at + 3 * CAP + 1, :] = sat[1, pl.ds(col, 1), :]


def load_state(press, depth, sat, rows):
    water, oil = sat[0, rows, :], sat[1, rows, :]
    return (press[rows, :], depth[rows, :]) + mobility(water, oil), water, oil


def chosen(role):
    if role is None:
        return True
    return (lax.axis_index("gx") == 0) == role


def stencil_kernel(cx, cy, first, last, role, *refs):
    @pl.when(chosen(role))
    def _():
        stencil_rows(cx, cy, first, last, *refs)


def stencil_rows(cx, cy, first, last, *refs):
    press, depth, sat, perm, pore = refs[:5]
    out = refs[-1]
    lanes = press.shape[1]
    lane = lax.broadcasted_iota(jnp.int32, (8, lanes), 1)
    sub = lax.broadcasted_iota(jnp.int32, (8, lanes), 0)
    chunks = cy // 8

    def at(a, c, shift=0):
        return pl.ds(pl.multiple_of(a * cy, 8) + (c * 8 + shift), 8)

    def flow_x(a, c, low):
        rows = at(a + 1, c)
        high, _, _ = load_state(press, depth, sat, rows)
        trans = harmonic(perm[0, at(a, c), :], perm[0, rows, :])
        return flux(low, high, trans)

    def one_row(a, carry, top):
        out_carry = []
        below = None
        for c in range(chunks):
            rows = at(a, c)
            mine, water, oil = load_state(press, depth, sat, rows)
            if top:
                net = [-carry[3 * c + f] for f in range(3)]
            else:
                up = flow_x(a, c, mine)
                out_carry += up
                net = [up[f] - carry[3 * c + f] for f in range(3)]
            ky = perm[1, rows, :]
            if c < chunks - 1:
                rows_up = at(a, c, 1)
                high, _, _ = load_state(press, depth, sat, rows_up)
                trans = harmonic(ky, perm[1, rows_up, :])
            else:
                high = tuple(pltpu.roll(v, 7, 0) for v in mine)
                trans = jnp.where(sub < 7, harmonic(ky, pltpu.roll(ky, 7, 0)), 0.0)
            flow = flux(mine, high, trans)
            for f in range(3):
                back = pltpu.roll(flow[f], 1, 0)
                first_row = jnp.zeros_like(back) if c == 0 else below[f]
                net[f] = net[f] + (flow[f] - jnp.where(sub == 0, first_row, back))
            below = [pltpu.roll(flow[f], 1, 0) for f in range(3)]
            kz = perm[2, rows, :]
            high = tuple(pltpu.roll(v, lanes - 1, 1) for v in mine)
            trans = jnp.where(lane < lanes - 1, harmonic(kz, pltpu.roll(kz, lanes - 1, 1)), 0.0)
            flow = flux(mine, high, trans)
            for f in range(3):
                net[f] = net[f] + (flow[f] - pltpu.roll(flow[f], 1, 1))
            scale = STEP / pore[rows, :]
            gas = 1.0 - water - oil
            for f, now in enumerate((water, oil, gas)):
                out[f, rows, :] = now - scale * net[f]
        return tuple(out_carry)

    if first == 0:
        carry = tuple(jnp.zeros((8, lanes), jnp.float32) for _ in range(3 * chunks))
    else:
        carry = []
        for c in range(chunks):
            low, _, _ = load_state(press, depth, sat, at(first - 1, c))
            carry += flow_x(first - 1, c, low)
        carry = tuple(carry)
    end = min(last, cx - 1)
    carry = lax.fori_loop(first, end, lambda a, value: one_row(a, value, False), carry, unroll=2)
    if last == cx:
        one_row(cx - 1, carry, True)


def halo_kernel(cx, cy, press, depth, sat, perm, hxa, hxb, hya, hyb):
    even_x = lax.rem(lax.axis_index("gx"), 2) == 0
    even_y = lax.rem(lax.axis_index("gy"), 2) == 0
    columns = cx * cy
    low, high = pl.ds(0, cy), pl.ds(columns - cy, cy)
    left, right = pl.ds(0, cx, stride=cy), pl.ds(cy - 1, cx, stride=cy)
    for field in range(5):

        def rows(where, dim):
            if field < 2:
                return (press, depth)[field][where, :]
            return sat[field - 2, where, :] if field < 4 else perm[dim, where, :]

        first, last = rows(low, 0), rows(high, 0)
        hxa[field] = jnp.where(even_x, last, first)
        hxb[field] = jnp.where(even_x, first, last)
        first, last = rows(left, 1), rows(right, 1)
        hya[field] = jnp.where(even_y, last, first)
        hyb[field] = jnp.where(even_y, first, last)


def blocks_of(own, got_a, got_b, plus, minus):
    listing = [(own, 0), (got_a, 0), (got_b, 0)]
    listing += [(plus, b) for b in range(3)] + [(minus, b) for b in range(3)]
    return listing


def fault_kernel(
    own, got_a, got_b, plus, minus, press, depth, sat, _,
    back_plus, back_minus, back_y, local,
):
    listing = blocks_of(own, got_a, got_b, plus, minus)
    targets = [(back_y, k * FLOW) for k in range(3)]
    targets += [(back_plus, k * FLOW) for k in range(3)]
    targets += [(back_minus, k * FLOW) for k in range(3)]
    for n, (ref, block) in enumerate(listing):
        meta = ref[META + block : META + block + 1, :].astype(jnp.int32)
        for rank in range(CAP):
            col = meta[0, rank]
            at = n * 4 * CAP + rank
            local[at : at + 1, :] = press[pl.ds(col, 1), :]
            local[at + CAP : at + CAP + 1, :] = depth[pl.ds(col, 1), :]
            local[at + 2 * CAP : at + 2 * CAP + 1, :] = sat[0, pl.ds(col, 1), :]
            local[at + 3 * CAP : at + 3 * CAP + 1, :] = sat[1, pl.ds(col, 1), :]
    for n, (ref, block) in enumerate(listing):
        far = [ref[block * BLOCK + f * CAP : block * BLOCK + (f + 1) * CAP, :] for f in range(5)]
        near = [local[(n * 4 + f) * CAP : (n * 4 + f + 1) * CAP, :] for f in range(4)]
        flow = flux(
            (far[0], far[1]) + mobility(far[2], far[3]),
            (near[0], near[1]) + mobility(near[2], near[3]),
            far[4],
        )
        out, row = targets[n]
        for f in range(3):
            out[row + f * CAP : row + (f + 1) * CAP, :] = flow[f]
    for out in (back_plus, back_minus, back_y):
        out[3 * FLOW : BACK, :] = jnp.zeros((BACK - 3 * FLOW, out.shape[1]), jnp.float32)


def edge_kernel(nx, ny, cx, cy, role, *refs):
    @pl.when(chosen(role))
    def _():
        edge_cells(nx, ny, cx, cy, *refs)


def edge_cells(
    nx, ny, cx, cy,
    own, got_a, got_b, plus, minus, back_plus, back_minus, back_y,
    hxa, hxb, hya, hyb, press, depth, sat, perm, pore, _,
    out,
):
    listing = blocks_of(own, got_a, got_b, plus, minus)
    sources = [(back_y, k * FLOW) for k in range(3)]
    sources += [(back_plus, k * FLOW) for k in range(3)]
    sources += [(back_minus, k * FLOW) for k in range(3)]
    home_x = lax.axis_index("gx")
    home_y = lax.axis_index("gy")
    columns = cx * cy

    def edge(first, second, dim, home, ends, rows_low, rows_high):
        even = lax.rem(home, 2) == 0
        for is_upper, rows in ((True, rows_high), (False, rows_low)):
            pick = even if is_upper else jnp.logical_not(even)
            far = [jnp.where(pick, first[f], second[f]) for f in range(5)]
            exists = (home < ends - 1) if is_upper else (home > 0)
            there = jnp.where(exists, 1.0, 0.0)
            mine, _, _ = load_state(press, depth, sat, rows)
            other = (far[0], far[1]) + mobility(far[2], far[3])
            trans = harmonic(perm[dim, rows, :], far[4]) * there
            if is_upper:
                flow = flux(mine, other, trans)
            else:
                flow = [-v for v in flux(other, mine, trans)]
            scale = STEP / pore[rows, :]
            for f in range(3):
                out[f, rows, :] = out[f, rows, :] - scale * flow[f]

    edge(hxa, hxb, 0, home_x, nx, pl.ds(0, cy), pl.ds(columns - cy, cy))
    edge(hya, hyb, 1, home_y, ny, pl.ds(0, cx, stride=cy), pl.ds(cy - 1, cx, stride=cy))
    for n, (ref, block) in enumerate(listing):
        meta = ref[META + block : META + block + 1, :].astype(jnp.int32)
        flows, row = sources[n]
        for rank in range(CAP):
            col = meta[0, rank]
            scale = STEP / pore[pl.ds(col, 1), :]
            for f in range(3):
                at = row + f * CAP + rank
                out[f, pl.ds(col, 1), :] = out[f, pl.ds(col, 1), :] + scale * flows[at : at + 1, :]


def finish_kernel(origin, back_y, from_up, from_down, from_a, from_b, pore, _, out, work, sem):
    slots = []
    for ty in range(3):
        for tx in range(3):
            if ty > 0:
                ref, row = (from_a, from_b)[ty - 1], tx * FLOW
            elif tx == 0:
                ref, row = back_y, 0
            else:
                ref, row = (from_up, from_down)[tx - 1], 0
            for rank in range(CAP):
                col = origin[(ty * 3 + tx) * CAP + rank]
                slots.append((ref, row + rank, pl.ds(col, 1), STEP / pore[pl.ds(col, 1), :]))
    copies = []
    for f in range(3):
        for ref, row, col, scale in slots:
            at = row + f * CAP
            work[f, col, :] = work[f, col, :] - scale * ref[at : at + 1, :]
        copies.append(pltpu.make_async_copy(work.at[f], out.at[f], sem.at[f]))
        copies[-1].start()
    for copy in copies:
        copy.wait()


def swapped(value, axis, kind):
    count = lax.axis_size(axis)
    route = []
    for i in range(count):
        j = i ^ 1 if kind == 0 else (((i + 1) ^ 1) - 1) % count
        route.append((i, j))
    return lax.ppermute(value, axis, route)


def swapped_inside(value):
    nx, ny = lax.axis_size("gx"), lax.axis_size("gy")
    route = []
    for i in range(nx):
        for j in range(ny):
            if i in (0, nx - 1):
                route.append((i * ny + j, i * ny + (j ^ 1)))
            else:
                route.append((i * ny + j, (((i + 1) ^ 1) - 1) * ny + j))
    return lax.ppermute(value, ("gx", "gy"), route)


def shifted(value, axis, step):
    count = lax.axis_size(axis)
    return lax.ppermute(value, axis, [(i, (i + step) % count) for i in range(count)])


def relay_kernel(own, got_a, got_b, plus, minus):
    parts = (own, got_a, got_b)
    for tx, out in ((1, plus), (2, minus)):
        low = tx * BLOCK
        for k, part in enumerate(parts):
            out[k * BLOCK : (k + 1) * BLOCK, :] = part[low : low + BLOCK, :]
            out[META + k : META + k + 1, :] = part[META + tx : META + tx + 1, :]
        out[META + 3 :, :] = jnp.zeros((1, out.shape[1]), jnp.float32)


def relay_back_kernel(back_y, from_up, from_down, _, back_a, back_b):
    for ty, out in ((1, back_a), (2, back_b)):
        low = ty * FLOW
        for k, part in enumerate((back_y, from_up, from_down)):
            out[k * FLOW : (k + 1) * FLOW, :] = part[low : low + FLOW, :]
        out[3 * FLOW :, :] = jnp.zeros((BACK - 3 * FLOW, out.shape[1]), jnp.float32)


def step(
    pressure, depth, saturation, permeability, pore_volume,
    fault_pairs, fault_kind, fault_count, fault_table,
):
    cx, cy, layers = pressure.shape
    columns = cx * cy
    nx, ny = lax.axis_size("gx"), lax.axis_size("gy")
    f32 = jnp.float32
    slots = 9 * CAP
    rows = fault_pairs.shape[0]

    def flat(array):
        return array.reshape(array.shape[:-3] + (columns, layers))

    def cells(array):
        return array.reshape(array.shape[:-2] + (cx, cy, layers))

    def outer(array):
        return pltpu.with_memory_space_constraint(array, HBM)

    def vmem(*dims):
        return VMEM(dims, f32)

    message, back, full = vmem(ROWS, layers), vmem(BACK, layers), vmem(3, columns, layers)
    halo_x, halo_y = vmem(5, cy, layers), vmem(5, cx, layers)
    own, msg_a, msg_b, press, deep, sat, origin = pl.pallas_call(
        functools.partial(pack_kernel, nx, ny),
        in_specs=[spec(HBM)] * 7,
        out_specs=[spec(VMEM)] * 6 + [spec(SMEM)],
        out_shape=[message] * 3
        + [vmem(columns, layers)] * 2 + [vmem(2, columns, layers)] + [SMEM((slots,), jnp.int32)],
        scratch_shapes=[
            SMEM((3, rows), jnp.int32), SMEM((rows,), jnp.int32), SMEM((1, 1), jnp.int32),
            SMEM((nx * ny,), jnp.int32),
            SMEM((slots,), jnp.int32), SMEM((slots,), jnp.int32),
            VMEM((fault_table.shape[0] + 8, layers), f32),
            pltpu.SemaphoreType.DMA((4,)), pltpu.SemaphoreType.DMA((3,)),
        ],
        compiler_params=params(),
        cost_estimate=cost(4_000_000),
        name="pack",
    )(*map(lambda a: a if a.size <= 1 else outer(a), (
        fault_pairs.T, fault_kind, fault_count.reshape(1, 1), fault_table,
        flat(pressure), flat(depth), flat(saturation),
    )))
    perm, pore = flat(permeability), flat(pore_volume)

    cuts = (cx * 3 // 8, cx * 5 // 8)

    def stencil(first, last, role, base):
        operands = [press, deep, sat, perm, pore] + ([] if base is None else [base])
        return pl.pallas_call(
            functools.partial(stencil_kernel, cx, cy, first, last, role),
            in_specs=[spec(VMEM)] * 5 + ([] if base is None else [spec(pl.ANY)]),
            out_specs=spec(VMEM),
            out_shape=full,
            input_output_aliases={} if base is None else {5: 0},
            compiler_params=params(),
            cost_estimate=cost(8_000_000 * (last - first) // 8),
            name="stencil",
        )(*operands)

    def edges(role, base):
        return pl.pallas_call(
            functools.partial(edge_kernel, nx, ny, cx, cy, role),
            in_specs=[spec(VMEM)] * 18,
            out_specs=spec(VMEM),
            out_shape=full,
            input_output_aliases={17: 0},
            compiler_params=params(),
            cost_estimate=cost(4_000_000),
            name="edge",
        )(own, got_a, got_b, plus, minus, back_plus, back_minus, back_y,
          hxa, hxb, hya, hyb, press, deep, sat, perm, pore, base)

    got_b = swapped(msg_b, "gy", 1)
    got_a = swapped(msg_a, "gy", 0)
    base = stencil(0, cuts[0], None, None)
    hxa, hxb, hya, hyb = pl.pallas_call(
        functools.partial(halo_kernel, cx, cy),
        in_specs=[spec(VMEM)] * 4,
        out_specs=[spec(VMEM)] * 4,
        out_shape=[halo_x] * 2 + [halo_y] * 2,
        compiler_params=params(),
        cost_estimate=cost(100_000),
        name="halo",
    )(press, deep, sat, perm)
    plus, minus = pl.pallas_call(
        relay_kernel,
        in_specs=[spec(VMEM)] * 3,
        out_specs=[spec(VMEM)] * 2,
        out_shape=[message] * 2,
        compiler_params=params(),
        cost_estimate=cost(100_000),
        name="relay",
    )(own, got_a, got_b)
    plus = shifted(plus, "gx", 1)
    minus = shifted(minus, "gx", -1)
    base = stencil(cuts[0], cuts[1], None, base)
    back_plus, back_minus, back_y = pl.pallas_call(
        fault_kernel,
        in_specs=[spec(VMEM)] * 8 + [spec(pl.ANY)],
        out_specs=[spec(VMEM)] * 3,
        out_shape=[back] * 3,
        scratch_shapes=[VMEM((slots * 4, layers), f32)],
        compiler_params=params(),
        cost_estimate=cost(2_000_000),
        name="fault",
    )(own, got_a, got_b, plus, minus, press, deep, sat, base)
    from_down = shifted(back_minus, "gx", 1)
    base = stencil(cuts[1], cx, True, base)
    from_up = shifted(back_plus, "gx", -1)
    hxa = swapped(hxa, "gx", 0)
    hxb = swapped_inside(hxb)
    hyb = swapped(hyb, "gy", 1)
    hya = swapped(hya, "gy", 0)
    base = stencil(cuts[1], cx, False, base)
    back_a, back_b = pl.pallas_call(
        relay_back_kernel,
        in_specs=[spec(VMEM)] * 3 + [spec(pl.ANY)],
        out_specs=[spec(VMEM)] * 2,
        out_shape=[back] * 2,
        compiler_params=params(),
        cost_estimate=cost(100_000),
        name="relay_back",
    )(back_y, from_up, from_down, base)
    from_b = swapped(back_b, "gy", 1)
    from_a = swapped(back_a, "gy", 0)
    base = edges(None, base)
    out, _ = pl.pallas_call(
        finish_kernel,
        in_specs=[spec(SMEM)] + [spec(VMEM)] * 7,
        out_specs=[spec(HBM), spec(VMEM)],
        out_shape=[jax.ShapeDtypeStruct((3, columns, layers), f32), full],
        input_output_aliases={7: 1},
        scratch_shapes=[pltpu.SemaphoreType.DMA((3,))],
        compiler_params=params(),
        cost_estimate=cost(2_000_000),
        name="finish",
    )(origin, back_y, from_up, from_down, from_a, from_b, pore, base)
    return cells(out)


def solution(mesh):
    in_specs = (
        P("gx", "gy", None),
        P("gx", "gy", None),
        P(None, "gx", "gy", None),
        P(None, "gx", "gy", None),
        P("gx", "gy", None),
        P(("gx", "gy"), None),
        P(("gx", "gy")),
        P(("gx", "gy")),
        P(),
    )
    out_specs = P(None, "gx", "gy", None)
    return jax.shard_map(step, mesh=mesh, in_specs=in_specs, out_specs=out_specs, check_vma=False)
```
